256 devices in a mesh: clip: 4 (over z_lo), vid: 8 (over y, core), aud: 8 (over x, z_hi).
Axes of the slice: x: 4, y: 4, z: 8 (z_hi: 2, z_lo: 4; z = z_hi * 4 + z_lo), core: 2. Of those that a mesh axis runs over, the one named last changes fastest.
Arguments:
- video_tokens: bfloat16 [4, 1024, 2048], P('clip', 'vid'), may hold values from -6 to 6
- audio_tokens: bfloat16 [4, 1024, 2048], P('clip', 'vid'), may hold values from -6 to 6
- qkv_video: bfloat16 [2048, 16, 384], P(None, 'aud'), may hold values from -0.125 to 0.125
- out_video: bfloat16 [16, 128, 2048], P('aud'), may hold values from -0.125 to 0.125
- qkv_audio: bfloat16 [2048, 16, 384], P(None, 'aud'), may hold values from -0.125 to 0.125
- out_audio: bfloat16 [16, 128, 2048], P('aud'), may hold values from -0.125 to 0.125
- gain_video: float32 [2048], replicated, may hold values from 0.5 to 1.5
- gain_audio: float32 [2048], replicated, may hold values from 0.5 to 1.5
- time_from: float32 [65, 2048], replicated, may hold values from -1.8 to 1.8
- time_to: float32 [65, 2048], replicated, may hold values from -1.8 to 1.8
- time_steps: int32 [4, 2], P('clip'), may hold values from 0 to 64, as said below
- windows: int32 [4, 2], P('clip'), may hold values from 32 to 128
- intersection: int32 [4, 32, 2], P('clip'), may hold values from 0 to 32, as said below
Outputs:
- d_video: bfloat16 [4, 1024, 2048], P('clip', 'vid')
- d_audio: bfloat16 [4, 1024, 2048], P('clip', 'vid')
- grad_qkv_video: float32 [2048, 16, 384], P(('clip', 'vid'), 'aud')
- grad_out_video: float32 [16, 128, 2048], P('aud', None, ('clip', 'vid'))
- grad_qkv_audio: float32 [2048, 16, 384], P(('clip', 'vid'), 'aud')
- grad_out_audio: float32 [16, 128, 2048], P('aud', None, ('clip', 'vid'))
The draws below stay inside these ranges and needn't reach their ends.
Inputs may be any that keep to these rules, and one draw needn't show every extreme that they name: `time_steps`: column 1 (m) is 1 or more and 2 * m <= column 0 (t) <= 64. `intersection`: entry b holds (lo, hi) with lo < hi, max(b * 32 - 128, 0) <= lo * 32 <= b * 32 and (hi - lo) * 32 <= 160.
All inputs are finite; a program needn't handle non-finite values.
Results may differ from the reference program's by a relative error of at most 0.029.
Values may be sent and summed in bfloat16 or wider, within the bound.
A program may use at most 128 MiB of HBM per device.

```python
import jax
import jax.numpy as jnp
from jax import lax

D = 2048
H = 16
DH = 128
TOK_DEV = 128
BLK = 32
TGRID = 64
STEPS = 2
NTOK = 1024
CLIPS = 4
NBLK = 32
N_VID = 8
N_AUD = 8


def draw_time_steps(key, part):
    first_key, second_key = jax.random.split(jax.random.fold_in(key, 11))
    stride = jax.random.randint(first_key, (CLIPS,), 1, TGRID // STEPS + 1)
    leeway = TGRID - STEPS * stride
    extra = jax.random.randint(second_key, (CLIPS,), 0, leeway + 1)
    return jnp.stack([STEPS * stride + extra, stride], 1).astype(jnp.int32)


def draw_intersection(key, part):
    per_shard = TOK_DEV // BLK
    first_key, second_key = jax.random.split(jax.random.fold_in(key, 23))
    home = jnp.arange(NBLK, dtype=jnp.int32)
    backward = jax.random.randint(first_key, (CLIPS, NBLK), 0, per_shard + 1)
    counts = jax.random.randint(second_key, (CLIPS, NBLK), 1, per_shard + 2)
    low_block = jnp.maximum(home[None, :] - backward, 0)
    high_block = jnp.minimum(low_block + counts, NBLK)
    return jnp.stack([low_block, high_block], -1).astype(jnp.int32)


def plant(drawn, rng, least, largest):
    shape = drawn.shape
    spot = [jax.random.randint(jax.random.fold_in(rng, axis), (), 0, shape[axis]) for axis in range(len(shape))]
    drawn = drawn.at[tuple(spot)].set(least)
    longest = shape.index(max(shape))
    spot[longest] = (spot[longest] + 1) % shape[longest]
    return drawn.at[tuple(spot)].set(largest)


def shard_levels(own_key, shape, cuts, smallest, high):
    loudness = 1.0
    for dim, parts in cuts:
        steps = jax.random.uniform(jax.random.fold_in(jax.random.fold_in(own_key, 6), dim), (parts,), jnp.float32, smallest / len(cuts), high / len(cuts))
        loudness = loudness * jnp.repeat(jnp.exp(steps), shape[dim] // parts).reshape((-1,) + (1,) * (len(shape) - 1 - dim))
    return loudness


def normal_values(own_key, dims, width, reach, cuts=(), kind=jnp.bfloat16):
    entries = width * jax.random.normal(own_key, dims, jnp.float32)
    if cuts:
        entries = entries * shard_levels(own_key, dims, cuts, -0.22, 0.18)
    return jnp.clip(entries, -reach, reach).astype(kind)


def setup_inputs(seed: int = 0) -> dict:
    splits = jax.random.split(jax.random.key(seed), 14)
    return {
        "video_tokens": normal_values(splits[0], (CLIPS, NTOK, D), 1.0, 6.0, ((0, 4), (1, 8))),
        "audio_tokens": normal_values(splits[1], (CLIPS, NTOK, D), 1.0, 6.0, ((0, 4), (1, 8))),
        "qkv_video": normal_values(splits[2], (D, H, 3 * DH), D ** -0.5, 0.125, ((1, 8),)),
        "out_video": normal_values(splits[3], (H, DH, D), (H * DH) ** -0.5, 0.125, ((0, 8),)),
        "qkv_audio": normal_values(splits[4], (D, H, 3 * DH), D ** -0.5, 0.125, ((1, 8),)),
        "out_audio": normal_values(splits[5], (H, DH, D), (H * DH) ** -0.5, 0.125, ((0, 8),)),
        "gain_video": jnp.clip(1.0 + 0.1 * jax.random.normal(splits[6], (D,), jnp.float32), 0.5, 1.5),
        "gain_audio": jnp.clip(1.0 + 0.1 * jax.random.normal(splits[7], (D,), jnp.float32), 0.5, 1.5),
        "time_from": normal_values(splits[8], (TGRID + 1, D), 0.3, 1.8, (), jnp.float32),
        "time_to": normal_values(splits[9], (TGRID + 1, D), 0.3, 1.8, (), jnp.float32),
        "time_steps": draw_time_steps(jax.random.fold_in(splits[13], 71), 0),
        "windows": plant(jax.random.randint(splits[11], (CLIPS, 2), TOK_DEV // 4, TOK_DEV + 1), jax.random.fold_in(splits[11], 1), TOK_DEV // 4, TOK_DEV).astype(jnp.int32),
        "intersection": draw_intersection(jax.random.fold_in(splits[13], 71), 0),
    }


EPSILON = 1e-06
PRECISE = lax.Precision.HIGHEST

def lookup(time_table, time_index):
    onehot = (jnp.arange(time_table.shape[0], dtype=jnp.int32) == time_index).astype(jnp.float32)
    return jnp.dot(onehot, time_table, precision=PRECISE)

def project_in(current, norm_gain, condition, weight):
    inv_rms = lax.rsqrt(lax.optimization_barrier(jnp.mean(current * current, -1, keepdims=True)) + EPSILON)
    modulation = norm_gain * (1.0 + condition)
    normed = (current * inv_rms * modulation).astype(jnp.bfloat16)
    qkv_rows = jnp.einsum('nd,dhe->nhe', normed.astype(jnp.float32), weight.astype(jnp.float32)).astype(jnp.bfloat16)
    return (normed, inv_rms, modulation, qkv_rows)

def attend(queries, key_rows, value_rows, key_mask):
    factor = DH ** (-0.5)
    scores = jnp.einsum('nhe,lhe->hnl', queries.astype(jnp.float32), key_rows.astype(jnp.float32)) * factor
    scores = jnp.where(key_mask[None], scores, -1e+30)
    shifted = jnp.exp(scores - lax.optimization_barrier(jnp.max(scores, -1, keepdims=True)))
    attn_prob = shifted / lax.optimization_barrier(jnp.sum(shifted, -1, keepdims=True))
    rounded = lax.optimization_barrier(attn_prob.astype(jnp.bfloat16))
    result = jnp.einsum('hnl,lhe->nhe', rounded.astype(jnp.float32), value_rows.astype(jnp.float32)).astype(jnp.bfloat16)
    return (result, attn_prob, rounded)

def attend_back(queries, key_rows, value_rows, attn_prob, rounded, grad_out):
    factor = DH ** (-0.5)
    grad_prob = jnp.einsum('nhe,lhe->hnl', grad_out.astype(jnp.float32), value_rows.astype(jnp.float32))
    center = lax.optimization_barrier(jnp.sum(attn_prob * grad_prob, -1, keepdims=True))
    dscore = lax.optimization_barrier((attn_prob * (grad_prob - center) * factor).astype(jnp.bfloat16))
    dscore_wide = dscore.astype(jnp.float32)
    dquery = jnp.einsum('hnl,lhe->nhe', dscore_wide, key_rows.astype(jnp.float32))
    key_grad = jnp.einsum('hnl,nhe->lhe', dscore_wide, queries.astype(jnp.float32))
    value_grad = jnp.einsum('hnl,nhe->lhe', rounded.astype(jnp.float32), grad_out.astype(jnp.float32))
    return (dquery, key_grad, value_grad)

def grouped_out(heads_out, weight):
    per_group = H // N_AUD
    partial_value = jnp.einsum('ngpe,gpef->gnf', heads_out.reshape(NTOK, N_AUD, per_group, DH).astype(jnp.float32), weight.reshape(N_AUD, per_group, DH, D).astype(jnp.float32))
    partial_value = lax.optimization_barrier(partial_value.astype(jnp.bfloat16))
    return lax.optimization_barrier(jnp.sum(partial_value.astype(jnp.float32), 0))

def grouped_back(grad_rows, weight):
    per_group = H // N_AUD
    partial_value = jnp.einsum('ngpe,dgpe->gnd', grad_rows.reshape(NTOK, N_AUD, per_group, 3 * DH).astype(jnp.float32), weight.reshape(D, N_AUD, per_group, 3 * DH).astype(jnp.float32))
    partial_value = lax.optimization_barrier(partial_value.astype(jnp.bfloat16))
    return lax.optimization_barrier(jnp.sum(partial_value.astype(jnp.float32), 0))

def norm_back(current, inv_rms, modulation, grad_normed):
    scaled = grad_normed * modulation
    return inv_rms * scaled - current * inv_rms ** 3 * lax.optimization_barrier(jnp.mean(scaled * current, -1, keepdims=True))

def blocked(pattern, left_side, right_side, out_shape):
    left_blocks = left_side.reshape((N_VID, TOK_DEV) + left_side.shape[1:])
    right_blocks = right_side.reshape((N_VID, TOK_DEV) + right_side.shape[1:])

    def accumulate(running, block_pair):
        partial_value = jnp.einsum(pattern, block_pair[0].astype(jnp.float32), block_pair[1].astype(jnp.float32))
        partial_value = lax.optimization_barrier(partial_value.astype(jnp.bfloat16)).astype(jnp.float32)
        return (running + partial_value, None)
    summed, unused = lax.scan(accumulate, jnp.zeros(out_shape, jnp.float32), (left_blocks, right_blocks))
    return summed

def build_masks(windows, intersection):
    position = jnp.arange(NTOK, dtype=jnp.int32)
    blocks = position // BLK
    distance = jnp.abs(position[:, None] - position[None, :])
    low_block = intersection[:, 0][blocks]
    high_block = intersection[:, 1][blocks]
    video_cross = (blocks[None, :] >= low_block[:, None]) & (blocks[None, :] < high_block[:, None])
    mask_video = jnp.concatenate([distance < windows[0], video_cross], 1)
    mask_audio = jnp.concatenate([video_cross.T, distance < windows[1]], 1)
    return (mask_video, mask_audio)

def network(video_now, audio_now, condition, key_masks, params):
    qkv_video, out_video, qkv_audio, out_audio, gain_video, gain_audio = params
    video_norm, video_inv, video_mod, video_rows = project_in(video_now, gain_video, condition, qkv_video)
    audio_norm, audio_inv, audio_mod, audio_rows = project_in(audio_now, gain_audio, condition, qkv_audio)
    key_rows = jnp.concatenate([video_rows[:, :, DH:2 * DH], audio_rows[:, :, DH:2 * DH]], 0)
    value_rows = jnp.concatenate([video_rows[:, :, 2 * DH:], audio_rows[:, :, 2 * DH:]], 0)
    video_out, video_prob, video_round = attend(video_rows[:, :, :DH], key_rows, value_rows, key_masks[0])
    audio_out, audio_prob, audio_round = attend(audio_rows[:, :, :DH], key_rows, value_rows, key_masks[1])
    video_field = grouped_out(video_out, out_video)
    audio_field = grouped_out(audio_out, out_audio)
    saved = (video_norm, video_inv, video_mod, video_rows, audio_norm, audio_inv, audio_mod, audio_rows, key_rows, value_rows, video_out, video_prob, video_round, audio_out, audio_prob, audio_round)
    return (video_field, audio_field, saved)

def one_clip(inputs, params, tables):
    video_tokens, audio_tokens, time_steps, windows, intersection = inputs
    qkv_video, out_video, qkv_audio, out_audio, gain_video, gain_audio = params
    time_from, time_to = tables
    key_masks = build_masks(windows, intersection)
    start_video = video_tokens.astype(jnp.float32)
    start_audio = audio_tokens.astype(jnp.float32)
    time_now = time_steps[0]
    stride = time_steps[1]
    euler_step = -stride.astype(jnp.float32) / TGRID
    video_now, audio_now = (start_video, start_audio)
    for teacher_step in range(STEPS):
        time_level = time_now - teacher_step * stride
        condition = lookup(time_from, time_level) + lookup(time_to, time_level)
        video_field, audio_field, unused = network(video_now, audio_now, condition, key_masks, params)
        video_now = video_now + euler_step * video_field
        audio_now = audio_now + euler_step * audio_field
    condition = lookup(time_from, time_now) + lookup(time_to, time_now - STEPS * stride)
    video_field, audio_field, saved = network(start_video, start_audio, condition, key_masks, params)
    video_norm, video_inv, video_mod, video_rows, audio_norm, audio_inv, audio_mod, audio_rows, key_rows, value_rows, video_out, video_prob, video_round, audio_out, audio_prob, audio_round = saved
    span_time = -(STEPS * stride).astype(jnp.float32) / TGRID
    video_diff = start_video + span_time * video_field - video_now
    audio_diff = start_audio + span_time * audio_field - audio_now
    video_grad = (span_time * video_diff).astype(jnp.bfloat16)
    audio_grad = (span_time * audio_diff).astype(jnp.bfloat16)
    video_dout = jnp.einsum('nf,hef->nhe', video_grad.astype(jnp.float32), out_video.astype(jnp.float32)).astype(jnp.bfloat16)
    audio_dout = jnp.einsum('nf,hef->nhe', audio_grad.astype(jnp.float32), out_audio.astype(jnp.float32)).astype(jnp.bfloat16)
    video_dq, video_dk, video_dv = attend_back(video_rows[:, :, :DH], key_rows, value_rows, video_prob, video_round, video_dout)
    audio_dq, audio_dk, audio_dv = attend_back(audio_rows[:, :, :DH], key_rows, value_rows, audio_prob, audio_round, audio_dout)
    key_grad = video_dk + audio_dk
    value_grad = video_dv + audio_dv
    video_dqkv = jnp.concatenate([video_dq, key_grad[:NTOK], value_grad[:NTOK]], -1).astype(jnp.bfloat16)
    audio_dqkv = jnp.concatenate([audio_dq, key_grad[NTOK:], value_grad[NTOK:]], -1).astype(jnp.bfloat16)
    video_back = grouped_back(video_dqkv, qkv_video)
    audio_back = grouped_back(audio_dqkv, qkv_audio)
    d_video = (video_diff + norm_back(start_video, video_inv, video_mod, video_back)).astype(jnp.bfloat16)
    d_audio = (audio_diff + norm_back(start_audio, audio_inv, audio_mod, audio_back)).astype(jnp.bfloat16)
    video_wqkv = blocked('nd,nhe->dhe', video_norm, video_dqkv, (D, H, 3 * DH))
    video_wout = blocked('nhe,nf->hef', video_out, video_grad, (H, DH, D))
    audio_wqkv = blocked('nd,nhe->dhe', audio_norm, audio_dqkv, (D, H, 3 * DH))
    audio_wout = blocked('nhe,nf->hef', audio_out, audio_grad, (H, DH, D))
    return (d_video, d_audio, video_wqkv, video_wout, audio_wqkv, audio_wout)

def reference(video_tokens, audio_tokens, qkv_video, out_video, qkv_audio, out_audio, gain_video, gain_audio, time_from, time_to, time_steps, windows, intersection):
    params = (qkv_video, out_video, qkv_audio, out_audio, gain_video, gain_audio)

    def per_clip(inputs):
        return one_clip(inputs, params, (time_from, time_to))
    results = lax.map(per_clip, (video_tokens, audio_tokens, time_steps, windows, intersection))
    return (results[0], results[1], lax.optimization_barrier(jnp.sum(results[2], 0)), lax.optimization_barrier(jnp.sum(results[3], 0)), lax.optimization_barrier(jnp.sum(results[4], 0)), lax.optimization_barrier(jnp.sum(results[5], 0)))
```

```python
import jax
import jax.numpy as jnp
from jax import lax
from jax.experimental import pallas as pl
from jax.experimental.pallas import tpu as pltpu
from jax.sharding import PartitionSpec as P

BLK = 32
TGRID = 64
STEPS = 2
EPSILON = 1e-06
MESH = pl.DeviceIdType.MESH
F32 = jnp.float32
BF16 = jnp.bfloat16
NT = (((1,), (1,)), ((), ()))
TN = (((0,), (0,)), ((), ()))
NN = (((1,), (0,)), ((), ()))
T1, ST, T2 = 0, 1, 2


def dot(a, b, dims):
    return lax.dot_general(a, b, dims, preferred_element_type=F32)


def kernel(
    xv, xa, mods, bias, wqv, wqa, wov, woa,
    dv_out, da_out, g_out,
    WQ, WO, N0, NS, NG, OB, OG, GS, GG, DQ, DG, QR, KV, PS, ACC, SB, R1, S2, R2, ZS, ZR, AG, DIFF,
    DO, DKV, DKS, DKR, W1, WR1, W2, WR2, SW, RW,
    w_sem, o_sem, kv_s, kv_r, ar_s, ar_r, ng_s, ng_r, og_s, og_r, gg_s, gg_r, dg_s, dg_r,
    w1_s, w1_r, w2_s, w2_r, sw_s, sw_r,
):
    v = lax.axis_index("vid")
    a = lax.axis_index("aud")
    c = lax.axis_index("clip")
    core = lax.rem(v, 2)
    yy = v // 2
    x = a // 2
    zh = lax.rem(a, 2)
    b0 = lax.rem(x, 2)
    b1 = x // 2
    q = lax.rem(b0 + b1, 2)
    near = (x + 1 - 2 * b0) * 2 + zh
    far = (3 - x) * 2 + zh
    across = a + 1 - 2 * zh
    first = (near, far)
    second = (far, near)
    keep1 = (q, b1)
    keep2 = (b1, b0)
    right = lax.rem(v + 1, 8)
    left = lax.rem(v + 7, 8)
    half0 = [pl.multiple_of(64 * k, 64) for k in keep1]
    half1 = [pl.multiple_of(64 * (1 - k), 64) for k in keep1]
    own = [pl.multiple_of(64 * k + 32 * j, 32) for k, j in zip(keep1, keep2)]
    other = [pl.multiple_of(64 * k + 32 * (1 - j), 32) for k, j in zip(keep1, keep2)]
    own_in = [pl.multiple_of(32 * j, 32) for j in keep2]
    other_in = [pl.multiple_of(32 * (1 - j), 32) for j in keep2]

    loads = [
        pltpu.make_async_copy(wqv, WQ.at[0], w_sem.at[0]),
        pltpu.make_async_copy(wqa, WQ.at[1], w_sem.at[1]),
        pltpu.make_async_copy(wov, WO.at[0], w_sem.at[2]),
        pltpu.make_async_copy(woa, WO.at[1], w_sem.at[3]),
    ]
    for load in loads:
        load.start()

    barrier = pltpu.get_barrier_semaphore()
    for d in range(1, 8):
        pl.semaphore_signal(barrier, 1, device_id={"vid": lax.rem(v + d, 8)}, device_id_type=MESH)
    for peer in (near, far, across):
        pl.semaphore_signal(barrier, 1, device_id={"aud": peer}, device_id_type=MESH)
    for d in range(1, 4):
        pl.semaphore_signal(barrier, 1, device_id={"clip": lax.rem(c + d, 4)}, device_id_type=MESH)

    pending = []

    def remote(src, dst, send, recv, device):
        return pltpu.make_async_remote_copy(
            src_ref=src, dst_ref=dst, send_sem=send, recv_sem=recv, device_id=device, device_id_type=MESH
        )

    def go(copy):
        copy.start()
        pending.append(copy)

    xs = (xv, xa)
    for m in range(2):

        def norm_rows(r, carry, m=m):
            rows = pl.ds(pl.multiple_of(r * 32, 32), 32)
            cur = xs[m][rows, :].astype(F32)
            inv = lax.rsqrt(jnp.mean(cur * cur, -1, keepdims=True) + EPSILON)
            scaled = cur * inv
            N0[m, 0, rows, :] = (scaled * mods[m : m + 1, :]).astype(BF16)
            student = (scaled * mods[2 + m : 3 + m, :]).astype(BF16)
            N0[m, 1, rows, :] = student
            for s in range(16):
                NS[m, s // 4, s % 4, rows, :] = student[:, 128 * s : 128 * s + 128]
            return carry

        lax.fori_loop(0, 4, norm_rows, 0)

    def store_qkv(net, m, rows):
        rounded = rows.astype(BF16)
        for h in range(2):
            QR[net, m, :, 128 * h : 128 * h + 128] = rounded[:, 384 * h : 384 * h + 128]
            KV[net, 1, m, :, 256 * h : 256 * h + 256] = rounded[:, 384 * h + 128 : 384 * h + 384]

    for m in range(2):
        loads[m].wait()
        both = dot(N0[m].reshape(256, 2048), WQ[m], NN)
        store_qkv(T1, m, both[:128])
        store_qkv(ST, m, both[128:])

    pl.semaphore_wait(barrier, 13)

    def kv_copies(net):
        return (
            remote(KV.at[net, 1], KV.at[net, 0], kv_s.at[2 * net], kv_r.at[2 * net], {"vid": right}),
            remote(KV.at[net, 1], KV.at[net, 2], kv_s.at[2 * net + 1], kv_r.at[2 * net + 1], {"vid": left}),
        )

    def kv_start(net):
        for copy in kv_copies(net):
            go(copy)

    def kv_wait(net):
        for copy in kv_copies(net):
            copy.wait_recv()

    kv_start(T1)
    kv_start(ST)

    def spread(src, dst, send, recv):
        for d in range(1, 8):
            peer = lax.rem(v + d, 8)
            go(remote(src(lax.rem(peer, 2), peer // 2), dst.at[v], send.at[peer], recv.at[v], {"vid": peer}))

    def collect(dst, send, recv):
        for d in range(1, 8):
            peer = lax.rem(v + d, 8)
            remote(dst.at[peer], dst.at[peer], send.at[peer], recv.at[peer], {"vid": peer}).wait_recv()

    NG[v] = NS[core, :, yy]
    spread(lambda k, y: NS.at[k, :, y], NG, ng_s, ng_r)

    factor = 128 ** (-0.5)

    def attention(net, m, save):
        for h in range(2):
            queries = QR[net, m, :, 128 * h : 128 * h + 128]
            keys = KV[net, :, :, :, 256 * h : 256 * h + 128].reshape(768, 128)
            values = KV[net, :, :, :, 256 * h + 128 : 256 * h + 256].reshape(768, 128)
            scores = dot(queries, keys, NT) * factor + bias[m]
            shifted = jnp.exp(scores - jnp.max(scores, -1, keepdims=True))
            prob = shifted * (1.0 / jnp.sum(shifted, -1, keepdims=True))
            if save:
                PS[2 * m + h] = prob
            OB[net, m, :, 128 * h : 128 * h + 128] = dot(prob.astype(BF16), values, NN).astype(BF16)

    def project_out(net, m):
        return dot(OB[net, m], WO[m], NN)

    def ar1(i, m):
        return remote(
            SB.at[i, m, pl.ds(half1[m], 64)], R1.at[i, m], ar_s.at[i, m, 0], ar_r.at[i, m, 0], {"aud": first[m]}
        )

    def ar2(i, m):
        return remote(S2.at[i, m], R2.at[i, m], ar_s.at[i, m, 1], ar_r.at[i, m, 1], {"aud": second[m]})

    def ar3(i, m):
        return remote(ZS.at[i, m], ZR.at[i, m], ar_s.at[i, m, 2], ar_r.at[i, m, 2], {"aud": across})

    def ag1(i, m):
        part = AG.at[i, m, pl.ds(own[m], 32)]
        return remote(part, part, ar_s.at[i, m, 3], ar_r.at[i, m, 3], {"aud": second[m]})

    def ag2(i, m):
        part = AG.at[i, m, pl.ds(half0[m], 64)]
        return remote(part, part, ar_s.at[i, m, 4], ar_r.at[i, m, 4], {"aud": first[m]})

    def ag1_recv(i, m):
        part = AG.at[i, m, pl.ds(other[m], 32)]
        remote(part, part, ar_s.at[i, m, 3], ar_r.at[i, m, 3], {"aud": second[m]}).wait_recv()

    def ag2_recv(i, m):
        part = AG.at[i, m, pl.ds(half1[m], 64)]
        remote(part, part, ar_s.at[i, m, 4], ar_r.at[i, m, 4], {"aud": first[m]}).wait_recv()

    def wide(ref):
        return ref.astype(F32)

    def reduce_1(i):
        for m in range(2):
            ar1(i, m).wait_recv()
            S2[i, m] = (
                wide(SB[i, m, pl.ds(other[m], 32), :]) + wide(R1[i, m, pl.ds(other_in[m], 32), :])
            ).astype(BF16)
            go(ar2(i, m))

    def reduce_2(i):
        for m in range(2):
            ar2(i, m).wait_recv()
            ZS[i, m] = (
                wide(SB[i, m, pl.ds(own[m], 32), :])
                + wide(R1[i, m, pl.ds(own_in[m], 32), :])
                + wide(R2[i, m])
            ).astype(BF16)
            go(ar3(i, m))

    def reduced(i, m):
        ar3(i, m).wait_recv()
        return wide(ZS[i, m]) + wide(ZR[i, m])

    def share_1(i):
        for m in range(2):
            ag1_recv(i, m)
            go(ag2(i, m))

    def share_2(i):
        for m in range(2):
            ag2_recv(i, m)

    for m in range(2):
        loads[2 + m].wait()
    kv_wait(T1)
    for m in range(2):
        attention(T1, m, False)
        field = project_out(T1, m)
        SB[0, m] = field.astype(BF16)
        ACC[m] = -field
        go(ar1(0, m))
    kv_wait(ST)
    attention(ST, 0, True)
    reduce_1(0)
    attention(ST, 1, True)
    OG[v] = OB[ST, core]
    spread(lambda k, y: OB.at[ST, k], OG, og_s, og_r)
    reduce_2(0)
    for m in range(2):
        ACC[m] = ACC[m] + 2.0 * project_out(ST, m)
    step = mods[6:7, :]
    for m in range(2):
        total = reduced(0, m)
        cur = wide(xs[m][pl.ds(own[m], 32), :]) + step * total
        inv = lax.rsqrt(jnp.mean(cur * cur, -1, keepdims=True) + EPSILON)
        AG[0, m, pl.ds(own[m], 32), :] = (cur * inv * mods[4 + m : 5 + m, :]).astype(BF16)
        go(ag1(0, m))
    share_1(0)
    share_2(0)

    for m in range(2):
        store_qkv(T2, m, dot(AG[0, m], WQ[m], NN))
    kv_start(T2)
    kv_wait(T2)
    for m in range(2):
        attention(T2, m, False)
        SB[1, m] = (ACC[m] - project_out(T2, m)).astype(BF16)
        go(ar1(1, m))
    collect(NG, ng_s, ng_r)
    collect(OG, og_s, og_r)
    reduce_1(1)
    reduce_2(1)
    for m in range(2):
        diff = step * reduced(1, m)
        DIFF[m] = diff
        AG[1, m, pl.ds(own[m], 32), :] = (2.0 * step * diff).astype(BF16)
        go(ag1(1, m))
    share_1(1)
    share_2(1)

    for m in range(2):
        for s in range(16):
            GS[m, s // 4, s % 4] = AG[1, m, :, 128 * s : 128 * s + 128]
    GG[v] = GS[core, :, yy]
    spread(lambda k, y: GS.at[k, :, y], GG, gg_s, gg_r)
    for m in range(2):
        DO[m] = dot(AG[1, m], WO[m], NT).astype(BF16)
    for m in range(2):
        for h in range(2):
            cols = slice(256 * h, 256 * h + 128)
            vcols = slice(256 * h + 128, 256 * h + 256)
            queries = QR[ST, m, :, 128 * h : 128 * h + 128]
            keys = KV[ST, :, :, :, cols].reshape(768, 128)
            values = KV[ST, :, :, :, vcols].reshape(768, 128)
            grad_out = DO[m, :, 128 * h : 128 * h + 128]
            prob = PS[2 * m + h]
            grad_prob = dot(grad_out, values, NT)
            center = jnp.sum(prob * grad_prob, -1, keepdims=True)
            dscore = (prob * (grad_prob - center) * factor).astype(BF16)
            DQ[m, :, 384 * h : 384 * h + 128] = dot(dscore, keys, NN).astype(BF16)
            dkey = dot(dscore, queries, TN).reshape(3, 2, 128, 128)
            dvalue = dot(prob.astype(BF16), grad_out, TN).reshape(3, 2, 128, 128)
            if m == 0:
                DKV[:, :, :, cols] = dkey
                DKV[:, :, :, vcols] = dvalue
            else:
                DKV[:, :, :, cols] = DKV[:, :, :, cols] + dkey
                DKV[:, :, :, vcols] = DKV[:, :, :, vcols] + dvalue
    DKS[0] = DKV[0].astype(BF16)
    DKS[1] = DKV[2].astype(BF16)
    edges = (
        remote(DKS.at[0], DKR.at[0], kv_s.at[6], kv_r.at[6], {"vid": left}),
        remote(DKS.at[1], DKR.at[1], kv_s.at[7], kv_r.at[7], {"vid": right}),
    )
    for copy in edges:
        go(copy)
    for copy in edges:
        copy.wait_recv()
    for m in range(2):
        owned = (DKV[1, m] + wide(DKR[0, m]) + wide(DKR[1, m])).astype(BF16)
        for h in range(2):
            DQ[m, :, 384 * h + 128 : 384 * h + 384] = owned[:, 256 * h : 256 * h + 256]
    DG[v] = DQ[core]
    spread(lambda k, y: DQ.at[k], DG, dg_s, dg_r)
    for m in range(2):
        SB[2, m] = dot(DQ[m], WQ[m], NT).astype(BF16)
        go(ar1(2, m))

    def clip_copies(send, got, s_sem, r_sem):
        for d in range(1, 4):
            peer = lax.rem(c + d, 4)
            go(remote(send.at[peer], got.at[c], s_sem.at[peer], r_sem.at[c], {"clip": peer}))

    def clip_sum(send, got, s_sem, r_sem):
        total = wide(send[c])
        for d in range(1, 4):
            peer = lax.rem(c + d, 4)
            remote(got.at[peer], got.at[peer], s_sem.at[peer], r_sem.at[peer], {"clip": peer}).wait_recv()
            total = total + wide(got[peer])
        return total

    collect(GG, gg_s, gg_r)
    o_all = OG[...].reshape(1024, 256)
    for s in range(4):
        W2[s] = dot(GG[:, s].reshape(1024, 128), o_all, TN).astype(BF16)
    clip_copies(W2, WR2, w2_s, w2_r)
    reduce_1(2)
    reduce_2(2)
    collect(DG, dg_s, dg_r)
    d_all = DG[...].reshape(1024, 768)
    for s in range(4):
        W1[s] = dot(NG[:, s].reshape(1024, 128), d_all, TN).astype(BF16)
    clip_copies(W1, WR1, w1_s, w1_r)
    for m in range(2):
        cur = wide(xs[m][pl.ds(own[m], 32), :])
        inv = lax.rsqrt(jnp.mean(cur * cur, -1, keepdims=True) + EPSILON)
        scaled = reduced(2, m) * mods[2 + m : 3 + m, :]
        back = inv * scaled - cur * (inv * inv * inv) * jnp.mean(scaled * cur, -1, keepdims=True)
        AG[2, m, pl.ds(own[m], 32), :] = (DIFF[m] + back).astype(BF16)
        go(ag1(2, m))
    share_1(2)
    mine = pl.ds(pl.multiple_of(64 * core, 64), 64)
    theirs = pl.ds(pl.multiple_of(64 * (1 - core), 64), 64)
    WS = ACC.at[0]
    WS[:, 768:1024] = clip_sum(W2, WR2, w2_s, w2_r)
    WS[:, 0:768] = clip_sum(W1, WR1, w1_s, w1_r)
    SW[...] = WS[theirs, 0:1024]
    swap = remote(SW, RW, sw_s, sw_r, {"vid": v + 1 - 2 * core})
    go(swap)
    g_out[core] = WS[mine, 0:1024]
    share_2(2)
    outs = (
        pltpu.make_async_copy(AG.at[2, 0], dv_out, o_sem.at[0]),
        pltpu.make_async_copy(AG.at[2, 1], da_out, o_sem.at[1]),
    )
    for copy in outs:
        copy.start()
    swap.wait_recv()
    g_out[1 - core] = RW[...]
    for copy in outs:
        copy.wait()
    for copy in pending:
        copy.wait_send()


def vm(shape, kind=BF16):
    return pltpu.VMEM(shape, kind)


def fused(xv, xa, mods, bias, wqv, wqa, wov, woa):
    dma = pltpu.SemaphoreType.DMA
    inside = pl.BlockSpec(memory_space=pltpu.VMEM)
    outside = pl.BlockSpec(memory_space=pl.ANY)
    return pl.pallas_call(
        kernel,
        out_shape=(
            jax.ShapeDtypeStruct((128, 2048), BF16),
            jax.ShapeDtypeStruct((128, 2048), BF16),
            jax.ShapeDtypeStruct((2, 64, 1024), F32),
        ),
        in_specs=[inside] * 4 + [outside] * 4,
        out_specs=(outside, outside, inside),
        scratch_shapes=[
            vm((2, 2048, 768)), vm((2, 256, 2048)), vm((2, 2, 128, 2048)), vm((2, 4, 4, 128, 128)),
            vm((8, 4, 128, 128)), vm((3, 2, 128, 256)), vm((8, 128, 256)), vm((2, 4, 4, 128, 128)),
            vm((8, 4, 128, 128)), vm((2, 128, 768)), vm((8, 128, 768)), vm((3, 2, 128, 256)),
            vm((3, 3, 2, 128, 512)), vm((4, 128, 768), F32), vm((2, 128, 2048), F32),
            vm((3, 2, 128, 2048)), vm((3, 2, 64, 2048)), vm((3, 2, 32, 2048)), vm((3, 2, 32, 2048)),
            vm((3, 2, 32, 2048)), vm((3, 2, 32, 2048)), vm((3, 2, 128, 2048)), vm((2, 32, 2048), F32),
            vm((2, 128, 256)), vm((3, 2, 128, 512), F32), vm((2, 2, 128, 512)), vm((2, 2, 128, 512)),
            vm((4, 128, 768)), vm((4, 128, 768)), vm((4, 128, 256)), vm((4, 128, 256)),
            vm((64, 1024), F32), vm((64, 1024), F32),
            dma((4,)), dma((2,)), dma((8,)), dma((8,)), dma((3, 2, 5)), dma((3, 2, 5)),
            dma((8,)), dma((8,)), dma((8,)), dma((8,)), dma((8,)), dma((8,)), dma((8,)), dma((8,)),
            dma((4,)), dma((4,)), dma((4,)), dma((4,)), dma, dma,
        ],
        compiler_params=pltpu.CompilerParams(
            collective_id=0, has_side_effects=True, vmem_limit_bytes=62 * 1024 * 1024
        ),
        name="step",
    )(xv, xa, mods, bias, wqv, wqa, wov, woa)


def local(
    video_tokens, audio_tokens, qkv_video, out_video, qkv_audio, out_audio, gain_video, gain_audio,
    time_from, time_to, time_steps, windows, intersection,
):
    tokens = video_tokens.shape[1]
    vid = lax.axis_index("vid")
    blocks = tokens // BLK
    qpos = jnp.arange(tokens, dtype=jnp.int32)[:, None, None]
    kpos = (jnp.arange(3, dtype=jnp.int32)[:, None] - 1) * tokens + jnp.arange(tokens, dtype=jnp.int32)[None, :]
    kpos = kpos[None]
    at = vid * tokens + kpos
    inside = (at >= 0) & (at < lax.axis_size("vid") * tokens)
    near_by = jnp.abs(qpos - kpos)
    qblk = vid * blocks + qpos // BLK
    kblk = at // BLK
    padded = jnp.pad(intersection[0], ((blocks, blocks), (0, 0)))
    ranges = lax.dynamic_slice_in_dim(padded, vid * blocks, 3 * blocks, axis=0)
    low = jnp.broadcast_to(ranges[:, 0][:, None], (3 * blocks, BLK)).reshape(1, 3, tokens)
    high = jnp.broadcast_to(ranges[:, 1][:, None], (3 * blocks, BLK)).reshape(1, 3, tokens)
    low_q = low[0, 1][:, None, None]
    high_q = high[0, 1][:, None, None]
    vv = inside & (near_by < windows[0, 0])
    va = inside & (kblk >= low_q) & (kblk < high_q)
    av = inside & (qblk >= low) & (qblk < high)
    aa = inside & (near_by < windows[0, 1])
    admit = jnp.stack([jnp.stack([vv, va], 2), jnp.stack([av, aa], 2)], 0)
    bias = jnp.where(admit, 0.0, -1e30).astype(F32).reshape(2, tokens, 6 * tokens)

    now = time_steps[0, 0]
    stride = time_steps[0, 1]

    def row(table, index):
        return lax.dynamic_index_in_dim(table, index, 0, keepdims=False)

    gains = jnp.stack([gain_video, gain_audio])
    first = row(time_from, now) + row(time_to, now)
    student = row(time_from, now) + row(time_to, now - STEPS * stride)
    second = row(time_from, now - stride) + row(time_to, now - stride)
    conds = jnp.stack([first, student, second])
    mods = (gains[None] * (1.0 + conds[:, None, :])).reshape(6, -1)
    step = jnp.broadcast_to(-stride.astype(F32) / TGRID, (2, mods.shape[1]))
    mods = jnp.concatenate([mods, step], 0)
    d_video, d_audio, grads = fused(
        video_tokens[0], audio_tokens[0], mods, bias,
        qkv_video.reshape(2048, 768), qkv_audio.reshape(2048, 768),
        out_video.reshape(256, 2048), out_audio.reshape(256, 2048),
    )

    def split(m):
        return grads[m, :, :768].reshape(64, 2, 384), grads[m, :, 768:].T.reshape(2, 128, 64)

    qv, ov = split(0)
    qa, oa = split(1)
    return d_video[None], d_audio[None], qv, ov, qa, oa


def solution(mesh):
    return jax.shard_map(
        local,
        mesh=mesh,
        in_specs=(
            P("clip", "vid", None), P("clip", "vid", None), P(None, "aud", None), P("aud", None, None),
            P(None, "aud", None), P("aud", None, None), P(), P(), P(), P(),
            P("clip", None), P("clip", None), P("clip", None, None),
        ),
        out_specs=(
            P("clip", "vid", None), P("clip", "vid", None), P(("clip", "vid"), "aud", None),
            P("aud", None, ("clip", "vid")), P(("clip", "vid"), "aud", None), P("aud", None, ("clip", "vid")),
        ),
        check_vma=False,
    )
```

```python
import jax
import jax.numpy as jnp
from jax import lax
from jax.experimental import pallas as pl
from jax.experimental.pallas import tpu as pltpu
from jax.sharding import PartitionSpec as P

BLK = 32
TGRID = 64
STEPS = 2
EPSILON = 1e-06
MESH = pl.DeviceIdType.MESH
F32 = jnp.float32
BF16 = jnp.bfloat16
NT = (((1,), (1,)), ((), ()))
TN = (((0,), (0,)), ((), ()))
NN = (((1,), (0,)), ((), ()))
T1, ST, T2 = 0, 1, 2
VMEM_LIMIT = 62 * 1024 * 1024


def dot(a, b, dims):
    return lax.dot_general(a, b, dims, preferred_element_type=F32)


def kernel(
    steps, windows, ranges, xv, xa, gv, ga, tf, tt, wqv, wqa, wov, woa,
    dv_out, da_out, qv_out, qa_out, ov_out, oa_out,
    WQ, WO, N0, NS, NG, NGT, OB, OG, GS, GG, DQ, DQS, DKVS, DGQ, DGK, QR, KV, PS, ACC,
    SB, R1, S2, R2, ZS, ZR, AG, DIFF, DO, DKV, DKS, DKR,
    WA, RA, WB, RB, WC, RC, MODS, BIAS,
    w_sem, o_sem, kv_s, kv_r, ar_s, ar_r, ng_s, ng_r, og_s, og_r, gg_s, gg_r,
    dq_s, dq_r, dk_s, dk_r, wa_s, wa_r, wb_s, wb_r, wc_s, wc_r,
):
    v = lax.axis_index("vid")
    a = lax.axis_index("aud")
    c = lax.axis_index("clip")
    core = lax.rem(v, 2)
    yy = v // 2
    x = a // 2
    zh = lax.rem(a, 2)
    b0 = lax.rem(x, 2)
    b1 = x // 2
    q = lax.rem(b0 + b1, 2)
    near = (x + 1 - 2 * b0) * 2 + zh
    far = (3 - x) * 2 + zh
    across = a + 1 - 2 * zh
    first = (near, far)
    second = (far, near)
    keep1 = (q, b1)
    keep2 = (b1, b0)
    keepf = (b1, 1 - b0)
    right = lax.rem(v + 1, 8)
    left = lax.rem(v + 7, 8)
    y_near = yy + 1 - 2 * lax.rem(yy, 2)
    y_far = 3 - yy
    y_one = (1 - core) * y_near + core * y_far
    y_two = core * y_near + (1 - core) * y_far
    y_last = 6 - yy - y_one - y_two
    mate = v + 1 - 2 * core

    def rows(value):
        return pl.ds(pl.multiple_of(value, 16), 16)

    chunks = [(g, m) for g in range(2) for m in range(2)]
    own, other, give, hold = {}, {}, {}, {}
    for g, m in chunks:
        base = 64 * g + 32 * keep1[m]
        away = 64 * g + 32 * (1 - keep1[m])
        own[g, m] = rows(base + 16 * keep2[m])
        other[g, m] = rows(base + 16 * (1 - keep2[m]))
        give[g, m] = rows(away + 16 * (1 - keepf[m]))
        hold[g, m] = rows(away + 16 * keepf[m])

    loads = [
        pltpu.make_async_copy(wqv, WQ.at[0], w_sem.at[0]),
        pltpu.make_async_copy(wqa, WQ.at[1], w_sem.at[1]),
        pltpu.make_async_copy(wov, WO.at[0], w_sem.at[2]),
        pltpu.make_async_copy(woa, WO.at[1], w_sem.at[3]),
    ]
    for load in loads:
        load.start()

    barrier = pltpu.get_barrier_semaphore()
    greet = [{"vid": lax.rem(v + d, 8)} for d in range(1, 8)]
    greet += [{"aud": peer} for peer in (near, far, across)]
    greet += [{"clip": lax.rem(c + d, 4), "vid": 2 * yy + k} for d in range(1, 4) for k in range(2)]
    for peer in greet:
        pl.semaphore_signal(barrier, 1, device_id=peer, device_id_type=MESH)

    pending = []

    def remote(src, dst, send, recv, device):
        return pltpu.make_async_remote_copy(
            src_ref=src, dst_ref=dst, send_sem=send, recv_sem=recv, device_id=device, device_id_type=MESH
        )

    def go(copy):
        copy.start()
        pending.append(copy)

    def wide(ref):
        return ref.astype(F32)

    now = steps[0, 0]
    stride = steps[0, 1]
    step = -stride.astype(F32) / TGRID
    conds = (
        tf[pl.ds(now, 1), :] + tt[pl.ds(now, 1), :],
        tf[pl.ds(now, 1), :] + tt[pl.ds(now - STEPS * stride, 1), :],
        tf[pl.ds(now - stride, 1), :] + tt[pl.ds(now - stride, 1), :],
    )
    gains = (gv, ga)
    for net in range(3):
        for m in range(2):
            MODS[2 * net + m : 2 * net + m + 1, :] = gains[m][...] * (1.0 + conds[net])

    xs = (xv, xa)

    def normed(net, m, r):
        part = pl.ds(pl.multiple_of(r * 32, 32), 32)
        cur = wide(xs[m][part, :])
        inv = lax.rsqrt(jnp.mean(cur * cur, -1, keepdims=True) + EPSILON)
        out = (cur * inv * MODS[2 * net + m : 2 * net + m + 1, :]).astype(BF16)
        N0[net, m, part, :] = out
        return part, out

    def store_qkv(net, m, value):
        rounded = value.astype(BF16)
        for h in range(2):
            QR[net, m, :, 128 * h : 128 * h + 128] = rounded[:, 384 * h : 384 * h + 128]
            KV[net, 1, m, :, 256 * h : 256 * h + 256] = rounded[:, 384 * h + 128 : 384 * h + 384]

    def kv_copies(net):
        return (
            remote(KV.at[net, 1], KV.at[net, 0], kv_s.at[2 * net], kv_r.at[2 * net], {"vid": right}),
            remote(KV.at[net, 1], KV.at[net, 2], kv_s.at[2 * net + 1], kv_r.at[2 * net + 1], {"vid": left}),
        )

    def kv_start(net):
        for copy in kv_copies(net):
            go(copy)

    def kv_wait(net):
        for copy in kv_copies(net):
            copy.wait_recv()

    for m in range(2):

        def norm_teacher(r, carry, m=m):
            normed(T1, m, r)
            return carry

        lax.fori_loop(0, 4, norm_teacher, 0)
    for m in range(2):
        loads[m].wait()
        store_qkv(T1, m, dot(N0[T1, m], WQ[m], NN))
    pl.semaphore_wait(barrier, len(greet))
    kv_start(T1)

    for m in range(2):

        def norm_student(r, carry, m=m):
            part, student = normed(ST, m, r)
            for s in range(16):
                NS[m, s // 4, s % 4, part, :] = student[:, 128 * s : 128 * s + 128]
            return carry

        lax.fori_loop(0, 4, norm_student, 0)
        store_qkv(ST, m, dot(N0[ST, m], WQ[m], NN))
    kv_start(ST)

    qpos = lax.broadcasted_iota(jnp.int32, (128, 128), 0)
    kpos = lax.broadcasted_iota(jnp.int32, (128, 128), 1)
    qblk = lax.broadcasted_iota(jnp.int32, (128, 1), 0) // BLK
    kblk = lax.broadcasted_iota(jnp.int32, (1, 128), 1) // BLK

    def spans(which, first_block, block_of):
        out = jnp.zeros(block_of.shape, jnp.int32)
        for i in range(4):
            at = jnp.clip(first_block + i, 0, 31)
            out = jnp.where(block_of == i, ranges[0, at, which], out)
        return out

    low_q = spans(0, 4 * v, qblk)
    high_q = spans(1, 4 * v, qblk)
    for slot in range(3):
        shard = v + slot - 1
        at = kpos + 128 * shard
        inside = (at >= 0) & (at < 1024)
        apart = jnp.abs(qpos - (kpos + 128 * (slot - 1)))
        keys_at = kblk + 4 * shard
        low_k = spans(0, 4 * shard, kblk)
        high_k = spans(1, 4 * shard, kblk)
        query_at = qblk + 4 * v
        tests = (
            (apart < windows[0, 0], (keys_at >= low_q) & (keys_at < high_q)),
            ((query_at >= low_k) & (query_at < high_k), apart < windows[0, 1]),
        )
        for m in range(2):
            for k in range(2):
                cols = slice(256 * slot + 128 * k, 256 * slot + 128 * k + 128)
                BIAS[m, :, cols] = jnp.where(inside & tests[m][k], 0.0, -1e30)

    def spread(src, dst, send, recv, offsets):
        for d in offsets:
            peer = 2 * lax.rem(yy + d[0], 4) + lax.rem(core + d[1], 2)
            go(remote(src(lax.rem(peer, 2), peer // 2), dst.at[v], send.at[peer], recv.at[v], {"vid": peer}))

    def collect(dst, send, recv):
        for d in range(1, 8):
            peer = lax.rem(v + d, 8)
            remote(dst.at[peer], dst.at[peer], send.at[peer], recv.at[peer], {"vid": peer}).wait_recv()

    close = [(0, 1), (1, 0), (3, 0), (1, 1), (3, 1)]
    distant = [(2, 0), (2, 1)]

    factor = 128 ** (-0.5)

    def attention(net, m, save):
        for h in range(2):
            queries = QR[net, m, :, 128 * h : 128 * h + 128]
            keys = KV[net, :, :, :, 256 * h : 256 * h + 128].reshape(768, 128)
            values = KV[net, :, :, :, 256 * h + 128 : 256 * h + 256].reshape(768, 128)
            scores = dot(queries, keys, NT) * factor + BIAS[m]
            shifted = jnp.exp(scores - jnp.max(scores, -1, keepdims=True))
            prob = shifted * (1.0 / jnp.sum(shifted, -1, keepdims=True))
            if save:
                PS[2 * m + h] = prob
            OB[net, m, :, 128 * h : 128 * h + 128] = dot(prob.astype(BF16), values, NN).astype(BF16)

    def project_out(net, m):
        return dot(OB[net, m], WO[m], NN)

    def aud(i, g, m, kind, src, dst, device):
        return remote(src, dst, ar_s.at[i, g, m, kind], ar_r.at[i, g, m, kind], {"aud": device})

    def sum_start(i, m):
        for kind, part in ((0, give), (1, hold)):
            for g in range(2):
                go(aud(i, g, m, kind, SB.at[i, m, part[g, m]], R1.at[i, g, m, kind], first[m]))

    def sum_1(i):
        for g, m in chunks:
            aud(i, g, m, 0, R1.at[i, g, m, 0], R1.at[i, g, m, 0], first[m]).wait_recv()
            S2[i, g, m] = (wide(SB[i, m, other[g, m], :]) + wide(R1[i, g, m, 0])).astype(BF16)
            go(aud(i, g, m, 2, S2.at[i, g, m], R2.at[i, g, m], second[m]))

    def sum_2(i):
        for g, m in chunks:
            aud(i, g, m, 1, R1.at[i, g, m, 1], R1.at[i, g, m, 1], first[m]).wait_recv()
            aud(i, g, m, 2, R2.at[i, g, m], R2.at[i, g, m], second[m]).wait_recv()
            ZS[i, g, m] = (
                wide(SB[i, m, own[g, m], :]) + wide(R1[i, g, m, 1]) + wide(R2[i, g, m])
            ).astype(BF16)
            go(aud(i, g, m, 3, ZS.at[i, g, m], ZR.at[i, g, m], across))

    def summed(i, g, m):
        aud(i, g, m, 3, ZR.at[i, g, m], ZR.at[i, g, m], across).wait_recv()
        return wide(ZS[i, g, m]) + wide(ZR[i, g, m])

    def share(i, g, m, value):
        AG[i, m, own[g, m], :] = value.astype(BF16)
        part = AG.at[i, m, own[g, m]]
        go(aud(i, g, m, 4, part, part, second[m]))
        go(aud(i, g, m, 5, part, part, first[m]))

    def share_on(i):
        for g, m in chunks:
            part = AG.at[i, m, other[g, m]]
            aud(i, g, m, 4, part, part, second[m]).wait_recv()
            go(aud(i, g, m, 6, part, part, first[m]))

    def share_end(i):
        for g, m in chunks:
            part = AG.at[i, m, hold[g, m]]
            aud(i, g, m, 5, part, part, first[m]).wait_recv()
            part = AG.at[i, m, give[g, m]]
            aud(i, g, m, 6, part, part, first[m]).wait_recv()

    for m in range(2):
        loads[2 + m].wait()
    kv_wait(T1)
    for m in range(2):
        attention(T1, m, False)
        field = project_out(T1, m)
        SB[0, m] = field.astype(BF16)
        ACC[m] = -field
        sum_start(0, m)
    kv_wait(ST)
    NG[v] = NS[core, :, yy]
    spread(lambda k, y: NS.at[k, :, y], NG, ng_s, ng_r, close + distant)
    attention(ST, 0, True)
    sum_1(0)
    attention(ST, 1, True)
    OG[v] = OB[ST, core]
    spread(lambda k, y: OB.at[ST, k], OG, og_s, og_r, close + distant)
    sum_2(0)
    for m in range(2):
        ACC[m] = ACC[m] + 2.0 * project_out(ST, m)
    for g, m in chunks:
        cur = wide(xs[m][own[g, m], :]) + step * summed(0, g, m)
        inv = lax.rsqrt(jnp.mean(cur * cur, -1, keepdims=True) + EPSILON)
        share(0, g, m, cur * inv * MODS[4 + m : 5 + m, :])
    share_on(0)
    share_end(0)

    for m in range(2):
        store_qkv(T2, m, dot(AG[0, m], WQ[m], NN))
    kv_start(T2)
    kv_wait(T2)
    for m in range(2):
        attention(T2, m, False)
        SB[1, m] = (ACC[m] - project_out(T2, m)).astype(BF16)
        sum_start(1, m)
    collect(NG, ng_s, ng_r)
    for s in range(4):
        NGT[128 * s : 128 * s + 128, :] = NG[:, s].reshape(1024, 128).T
    sum_1(1)
    collect(OG, og_s, og_r)
    sum_2(1)
    for g, m in chunks:
        diff = step * summed(1, g, m)
        DIFF[g, m] = diff
        share(1, g, m, 2.0 * step * diff)
    share_on(1)
    share_end(1)

    for m in range(2):
        for s in range(16):
            GS[m, s // 4, s % 4] = AG[1, m, :, 128 * s : 128 * s + 128]
    GG[v] = GS[core, :, yy]
    spread(lambda k, y: GS.at[k, :, y], GG, gg_s, gg_r, close)
    for m in range(2):
        DO[m] = dot(AG[1, m], WO[m], NT).astype(BF16)
    for m in range(2):
        for h in range(2):
            cols = slice(256 * h, 256 * h + 128)
            vcols = slice(256 * h + 128, 256 * h + 256)
            queries = QR[ST, m, :, 128 * h : 128 * h + 128]
            keys = KV[ST, :, :, :, cols].reshape(768, 128)
            values = KV[ST, :, :, :, vcols].reshape(768, 128)
            grad_out = DO[m, :, 128 * h : 128 * h + 128]
            prob = PS[2 * m + h]
            grad_prob = dot(grad_out, values, NT)
            center = jnp.sum(prob * grad_prob, -1, keepdims=True)
            dscore = (prob * (grad_prob - center) * factor).astype(BF16)
            dquery = dot(dscore, keys, NN).astype(BF16)
            DQ[m, :, 384 * h : 384 * h + 128] = dquery
            DQS[m, :, 128 * h : 128 * h + 128] = dquery
            dkey = dot(dscore, queries, TN).reshape(3, 2, 128, 128)
            dvalue = dot(prob.astype(BF16), grad_out, TN).reshape(3, 2, 128, 128)
            if m == 0:
                DKV[:, :, :, cols] = dkey
                DKV[:, :, :, vcols] = dvalue
            else:
                DKV[:, :, :, cols] = DKV[:, :, :, cols] + dkey
                DKV[:, :, :, vcols] = DKV[:, :, :, vcols] + dvalue
    DKS[0] = DKV[0].astype(BF16)
    DKS[1] = DKV[2].astype(BF16)
    edges = (
        remote(DKS.at[0], DKR.at[0], kv_s.at[6], kv_r.at[6], {"vid": left}),
        remote(DKS.at[1], DKR.at[1], kv_s.at[7], kv_r.at[7], {"vid": right}),
    )
    for copy in edges:
        go(copy)

    def line_start(src, dst, s_sem, r_sem):
        dst[yy, core] = src[core]
        go(remote(src.at[1 - core], dst.at[yy, core], s_sem.at[0], r_sem.at[0], {"vid": mate}))

    def line_send(dst, s_sem, r_sem):
        part = dst.at[yy, 1 - core]
        remote(part, part, s_sem.at[0], r_sem.at[0], {"vid": mate}).wait_recv()
        part = dst.at[yy]
        go(remote(part, part, s_sem.at[1], r_sem.at[1], {"vid": 2 * y_one + core}))
        go(remote(part, part, s_sem.at[2], r_sem.at[2], {"vid": 2 * y_two + core}))

    def line_on(dst, s_sem, r_sem):
        part = dst.at[y_one]
        remote(part, part, s_sem.at[1], r_sem.at[1], {"vid": 2 * y_one + core}).wait_recv()
        go(remote(part, part, s_sem.at[3], r_sem.at[3], {"vid": 2 * y_two + core}))

    def line_end(dst, s_sem, r_sem):
        part = dst.at[y_two]
        remote(part, part, s_sem.at[2], r_sem.at[2], {"vid": 2 * y_two + core}).wait_recv()
        part = dst.at[y_last]
        remote(part, part, s_sem.at[3], r_sem.at[3], {"vid": 2 * y_two + core}).wait_recv()

    line_start(DQS, DGQ, dq_s, dq_r)
    line_send(DGQ, dq_s, dq_r)
    for copy in edges:
        copy.wait_recv()
    for m in range(2):
        owned = (DKV[1, m] + wide(DKR[0, m]) + wide(DKR[1, m])).astype(BF16)
        DKVS[m] = owned
        for h in range(2):
            DQ[m, :, 384 * h + 128 : 384 * h + 384] = owned[:, 256 * h : 256 * h + 256]
    line_start(DKVS, DGK, dk_s, dk_r)
    SB[2, 0] = dot(DQ[0], WQ[0], NT).astype(BF16)
    sum_start(2, 0)
    line_send(DGK, dk_s, dk_r)
    SB[2, 1] = dot(DQ[1], WQ[1], NT).astype(BF16)
    sum_start(2, 1)
    line_on(DGQ, dq_s, dq_r)
    spread(lambda k, y: GS.at[k, :, y], GG, gg_s, gg_r, distant)

    def clip_start(send, got, s_sem, r_sem):
        for d in range(4):
            peer = lax.rem(c + d, 4)
            for k in range(2):
                to = lax.rem(core + 1 - k, 2)
                half = pl.ds(pl.multiple_of(64 * to, 64), 64)
                if d == 0 and k == 1:
                    got[core, c] = send[c, half, :]
                else:
                    device = {"clip": peer, "vid": 2 * yy + to}
                    go(remote(send.at[peer, half], got.at[core, c], s_sem.at[to, peer], r_sem.at[core, c], device))

    def clip_end(got, s_sem, r_sem):
        for d in range(4):
            peer = lax.rem(c + d, 4)
            for k in range(2):
                if d == 0 and k == 1:
                    continue
                to = lax.rem(core + 1 - k, 2)
                part = got.at[to, peer]
                device = {"clip": peer, "vid": 2 * yy + to}
                remote(part, part, s_sem.at[to, peer], r_sem.at[to, peer], device).wait_recv()

    def clip_sum(got, m):
        return (wide(got[m, 0]) + wide(got[m, 1])) + (wide(got[m, 2]) + wide(got[m, 3]))

    sum_1(2)
    line_on(DGK, dk_s, dk_r)
    line_end(DGQ, dq_s, dq_r)
    dq_all = DGQ[...].reshape(1024, 256)
    WA[...] = dot(NGT[...], dq_all, NN).astype(BF16).reshape(4, 128, 256)
    clip_start(WA, RA, wa_s, wa_r)
    sum_2(2)
    line_end(DGK, dk_s, dk_r)
    dk_all = DGK[...].reshape(1024, 512)
    WB[...] = dot(NGT[...], dk_all, NN).astype(BF16).reshape(4, 128, 512)
    clip_start(WB, RB, wb_s, wb_r)
    for g, m in chunks:
        cur = wide(xs[m][own[g, m], :])
        inv = lax.rsqrt(jnp.mean(cur * cur, -1, keepdims=True) + EPSILON)
        scaled = summed(2, g, m) * MODS[2 + m : 3 + m, :]
        back = inv * scaled - cur * (inv * inv * inv) * jnp.mean(scaled * cur, -1, keepdims=True)
        share(2, g, m, DIFF[g, m] + back)
    collect(GG, gg_s, gg_r)
    o_all = OG[...].reshape(1024, 256)
    for s in range(4):
        WC[s] = dot(GG[:, s].reshape(1024, 128), o_all, TN).astype(BF16)
    clip_start(WC, RC, wc_s, wc_r)
    share_on(2)
    q_outs = (qv_out, qa_out)
    o_outs = (ov_out, oa_out)
    clip_end(RA, wa_s, wa_r)
    for m in range(2):
        total = clip_sum(RA, m)
        for h in range(2):
            q_outs[m][:, h, 0:128] = total[:, 128 * h : 128 * h + 128]
    share_end(2)
    outs = (
        pltpu.make_async_copy(AG.at[2, 0], dv_out, o_sem.at[0]),
        pltpu.make_async_copy(AG.at[2, 1], da_out, o_sem.at[1]),
    )
    for copy in outs:
        copy.start()
    clip_end(RB, wb_s, wb_r)
    for m in range(2):
        total = clip_sum(RB, m)
        for h in range(2):
            q_outs[m][:, h, 128:384] = total[:, 256 * h : 256 * h + 256]
    clip_end(RC, wc_s, wc_r)
    for m in range(2):
        total = clip_sum(RC, m)
        for h in range(2):
            o_outs[m][h] = total[:, 128 * h : 128 * h + 128]
    for copy in outs:
        copy.wait()
    for copy in pending:
        copy.wait_send()


def vm(shape, kind=BF16):
    return pltpu.VMEM(shape, kind)


def fused(*operands):
    dma = pltpu.SemaphoreType.DMA
    inside = pl.BlockSpec(memory_space=pltpu.VMEM)
    scalar = pl.BlockSpec(memory_space=pltpu.SMEM)
    outside = pl.BlockSpec(memory_space=pl.ANY)
    shape = jax.ShapeDtypeStruct
    return pl.pallas_call(
        kernel,
        out_shape=(
            shape((128, 2048), BF16), shape((128, 2048), BF16), shape((64, 2, 384), F32),
            shape((64, 2, 384), F32), shape((2, 64, 128), F32), shape((2, 64, 128), F32),
        ),
        in_specs=[scalar] * 3 + [inside] * 6 + [outside] * 4,
        out_specs=(outside, outside, inside, inside, inside, inside),
        scratch_shapes=[
            vm((2, 2048, 768)), vm((2, 256, 2048)), vm((2, 2, 128, 2048)), vm((2, 4, 4, 128, 128)),
            vm((8, 4, 128, 128)), vm((512, 1024)), vm((3, 2, 128, 256)), vm((8, 128, 256)),
            vm((2, 4, 4, 128, 128)), vm((8, 4, 128, 128)), vm((2, 128, 768)), vm((2, 128, 256)),
            vm((2, 128, 512)), vm((4, 2, 128, 256)), vm((4, 2, 128, 512)), vm((3, 2, 128, 256)),
            vm((3, 3, 2, 128, 512)), vm((4, 128, 768), F32), vm((2, 128, 2048), F32),
            vm((3, 2, 128, 2048)), vm((3, 2, 2, 2, 16, 2048)), vm((3, 2, 2, 16, 2048)),
            vm((3, 2, 2, 16, 2048)), vm((3, 2, 2, 16, 2048)), vm((3, 2, 2, 16, 2048)),
            vm((3, 2, 128, 2048)), vm((2, 2, 16, 2048), F32), vm((2, 128, 256)),
            vm((3, 2, 128, 512), F32), vm((2, 2, 128, 512)), vm((2, 2, 128, 512)),
            vm((4, 128, 256)), vm((2, 4, 64, 256)), vm((4, 128, 512)), vm((2, 4, 64, 512)),
            vm((4, 128, 256)), vm((2, 4, 64, 256)), vm((8, 2048), F32), vm((2, 128, 768), F32),
            dma((4,)), dma((2,)), dma((8,)), dma((8,)), dma((3, 2, 2, 7)), dma((3, 2, 2, 7)),
            dma((8,)), dma((8,)), dma((8,)), dma((8,)), dma((8,)), dma((8,)),
            dma((4,)), dma((4,)), dma((4,)), dma((4,)),
            dma((2, 4)), dma((2, 4)), dma((2, 4)), dma((2, 4)), dma((2, 4)), dma((2, 4)),
        ],
        compiler_params=pltpu.CompilerParams(
            collective_id=0, has_side_effects=True, vmem_limit_bytes=VMEM_LIMIT
        ),
        name="step",
    )(*operands)


def local(
    video_tokens, audio_tokens, qkv_video, out_video, qkv_audio, out_audio, gain_video, gain_audio,
    time_from, time_to, time_steps, windows, intersection,
):
    d_video, d_audio, qv, qa, ov, oa = fused(
        time_steps, windows, intersection, video_tokens[0], audio_tokens[0],
        gain_video.reshape(1, 2048), gain_audio.reshape(1, 2048), time_from, time_to,
        qkv_video.reshape(2048, 768), qkv_audio.reshape(2048, 768),
        out_video.reshape(256, 2048), out_audio.reshape(256, 2048),
    )
    return d_video[None], d_audio[None], qv, ov.swapaxes(1, 2), qa, oa.swapaxes(1, 2)


def solution(mesh):
    return jax.shard_map(
        local,
        mesh=mesh,
        in_specs=(
            P("clip", "vid", None), P("clip", "vid", None), P(None, "aud", None), P("aud", None, None),
            P(None, "aud", None), P("aud", None, None), P(), P(), P(), P(),
            P("clip", None), P("clip", None), P("clip", None, None),
        ),
        out_specs=(
            P("clip", "vid", None), P("clip", "vid", None), P(("clip", "vid"), "aud", None),
            P("aud", None, ("clip", "vid")), P(("clip", "vid"), "aud", None), P("aud", None, ("clip", "vid")),
        ),
        check_vma=False,
    )
```

```python
import jax
import jax.numpy as jnp
from jax import lax
from jax.experimental import pallas as pl
from jax.experimental.pallas import tpu as pltpu
from jax.sharding import PartitionSpec as P

BLK = 32
TGRID = 64
STEPS = 2
EPSILON = 1e-06
MESH = pl.DeviceIdType.MESH
F32 = jnp.float32
BF16 = jnp.bfloat16
NT = (((1,), (1,)), ((), ()))
TN = (((0,), (0,)), ((), ()))
NN = (((1,), (0,)), ((), ()))
T1, ST, T2 = 0, 1, 2
VMEM_LIMIT = 62 * 1024 * 1024


def dot(a, b, dims):
    return lax.dot_general(a, b, dims, preferred_element_type=F32)


def kernel(
    steps, windows, ranges, xv, xa, gv, ga, tf, tt, wqv, wqa, wov, woa,
    dv_out, da_out, qv_out, qa_out, ov_out, oa_out,
    WQ, WO, N0, NS, NG, NGT, OB, OG, GS, GG, DQ, DQS, DG, QR, KV, PS, ACC,
    SB, R1, S2, R2, ZS, ZR, AG, DIFF, DO, DKV, DKS, DKR,
    W, WR, WS, WF, MODS, BIAS,
    w_sem, o_sem, kv_s, kv_r, ar_s, ar_r, ng_s, ng_r, og_s, og_r, gg_s, gg_r,
    dg_s, dg_r, cl_s, cl_r, wf_r,
):
    v = lax.axis_index("vid")
    a = lax.axis_index("aud")
    c = lax.axis_index("clip")
    core = lax.rem(v, 2)
    yy = v // 2
    x = a // 2
    zh = lax.rem(a, 2)
    b0 = lax.rem(x, 2)
    b1 = x // 2
    q = lax.rem(b0 + b1, 2)
    near = (x + 1 - 2 * b0) * 2 + zh
    far = (3 - x) * 2 + zh
    across = a + 1 - 2 * zh
    first = (near, far)
    second = (far, near)
    keep1 = (q, b1)
    keep2 = (b1, b0)
    keepf = (b1, 1 - b0)
    right = lax.rem(v + 1, 8)
    left = lax.rem(v + 7, 8)
    y_near = yy + 1 - 2 * lax.rem(yy, 2)
    y_far = 3 - yy
    y_one = (1 - core) * y_near + core * y_far
    y_two = core * y_near + (1 - core) * y_far
    y_last = 6 - yy - y_one - y_two
    mate = v + 1 - 2 * core

    def rows(value):
        return pl.ds(pl.multiple_of(value, 16), 16)

    chunks = [(g, m) for g in range(2) for m in range(2)]
    own, other, give, hold = {}, {}, {}, {}
    for g, m in chunks:
        base = 64 * g + 32 * keep1[m]
        away = 64 * g + 32 * (1 - keep1[m])
        own[g, m] = rows(base + 16 * keep2[m])
        other[g, m] = rows(base + 16 * (1 - keep2[m]))
        give[g, m] = rows(away + 16 * (1 - keepf[m]))
        hold[g, m] = rows(away + 16 * keepf[m])

    loads = [
        pltpu.make_async_copy(wqv, WQ.at[0], w_sem.at[0]),
        pltpu.make_async_copy(wqa, WQ.at[1], w_sem.at[1]),
        pltpu.make_async_copy(wov, WO.at[0], w_sem.at[2]),
        pltpu.make_async_copy(woa, WO.at[1], w_sem.at[3]),
    ]
    for load in loads:
        load.start()

    barrier = pltpu.get_barrier_semaphore()
    greet = [{"vid": lax.rem(v + d, 8)} for d in range(1, 8)]
    greet += [{"aud": peer} for peer in (near, far, across)]
    greet += [{"clip": c + 1 - 2 * lax.rem(c, 2)}]
    greet += [{"clip": lax.rem(c + 2, 4), "vid": 2 * yy + k} for k in range(2)]
    for peer in greet:
        pl.semaphore_signal(barrier, 1, device_id=peer, device_id_type=MESH)

    pending = []

    def remote(src, dst, send, recv, device):
        return pltpu.make_async_remote_copy(
            src_ref=src, dst_ref=dst, send_sem=send, recv_sem=recv, device_id=device, device_id_type=MESH
        )

    def go(copy):
        copy.start()
        pending.append(copy)

    def wide(ref):
        return ref.astype(F32)

    now = steps[0, 0]
    stride = steps[0, 1]
    step = -stride.astype(F32) / TGRID
    conds = (
        tf[pl.ds(now, 1), :] + tt[pl.ds(now, 1), :],
        tf[pl.ds(now, 1), :] + tt[pl.ds(now - STEPS * stride, 1), :],
        tf[pl.ds(now - stride, 1), :] + tt[pl.ds(now - stride, 1), :],
    )
    gains = (gv, ga)
    for net in range(3):
        for m in range(2):
            MODS[2 * net + m : 2 * net + m + 1, :] = gains[m][...] * (1.0 + conds[net])

    xs = (xv, xa)

    def normed(net, m, r):
        part = pl.ds(pl.multiple_of(r * 32, 32), 32)
        cur = wide(xs[m][part, :])
        inv = lax.rsqrt(jnp.mean(cur * cur, -1, keepdims=True) + EPSILON)
        out = (cur * inv * MODS[2 * net + m : 2 * net + m + 1, :]).astype(BF16)
        N0[net, m, part, :] = out
        return part, out

    def store_qkv(net, m, value):
        rounded = value.astype(BF16)
        for h in range(2):
            QR[net, m, :, 128 * h : 128 * h + 128] = rounded[:, 384 * h : 384 * h + 128]
            KV[net, 1, m, :, 256 * h : 256 * h + 256] = rounded[:, 384 * h + 128 : 384 * h + 384]

    def kv_copies(net):
        return (
            remote(KV.at[net, 1], KV.at[net, 0], kv_s.at[2 * net], kv_r.at[2 * net], {"vid": right}),
            remote(KV.at[net, 1], KV.at[net, 2], kv_s.at[2 * net + 1], kv_r.at[2 * net + 1], {"vid": left}),
        )

    def kv_start(net):
        for copy in kv_copies(net):
            go(copy)

    def kv_wait(net):
        for copy in kv_copies(net):
            copy.wait_recv()

    for m in range(2):

        def norm_teacher(r, carry, m=m):
            normed(T1, m, r)
            return carry

        lax.fori_loop(0, 4, norm_teacher, 0)
    for m in range(2):
        loads[m].wait()
        store_qkv(T1, m, dot(N0[T1, m], WQ[m], NN))
    pl.semaphore_wait(barrier, len(greet))
    kv_start(T1)

    for m in range(2):

        def norm_student(r, carry, m=m):
            part, student = normed(ST, m, r)
            for s in range(16):
                NS[m, s // 4, s % 4, part, :] = student[:, 128 * s : 128 * s + 128]
            return carry

        lax.fori_loop(0, 4, norm_student, 0)
        store_qkv(ST, m, dot(N0[ST, m], WQ[m], NN))
    kv_start(ST)

    qpos = lax.broadcasted_iota(jnp.int32, (128, 128), 0)
    kpos = lax.broadcasted_iota(jnp.int32, (128, 128), 1)
    qblk = lax.broadcasted_iota(jnp.int32, (128, 1), 0) // BLK
    kblk = lax.broadcasted_iota(jnp.int32, (1, 128), 1) // BLK

    def spans(which, first_block, block_of):
        out = jnp.zeros(block_of.shape, jnp.int32)
        for i in range(4):
            at = jnp.clip(first_block + i, 0, 31)
            out = jnp.where(block_of == i, ranges[0, which, at], out)
        return out

    low_q = spans(0, 4 * v, qblk)
    high_q = spans(1, 4 * v, qblk)
    for slot in range(3):
        shard = v + slot - 1
        at = kpos + 128 * shard
        inside = (at >= 0) & (at < 1024)
        apart = jnp.abs(qpos - (kpos + 128 * (slot - 1)))
        keys_at = kblk + 4 * shard
        low_k = spans(0, 4 * shard, kblk)
        high_k = spans(1, 4 * shard, kblk)
        query_at = qblk + 4 * v
        tests = (
            (apart < windows[0, 0], (keys_at >= low_q) & (keys_at < high_q)),
            ((query_at >= low_k) & (query_at < high_k), apart < windows[0, 1]),
        )
        for m in range(2):
            for k in range(2):
                cols = slice(256 * slot + 128 * k, 256 * slot + 128 * k + 128)
                BIAS[m, :, cols] = jnp.where(inside & tests[m][k], 0.0, -1e30)

    def spread(src, dst, send, recv, offsets):
        for d in offsets:
            peer = 2 * lax.rem(yy + d[0], 4) + lax.rem(core + d[1], 2)
            go(remote(src(lax.rem(peer, 2), peer // 2), dst.at[v], send.at[peer], recv.at[v], {"vid": peer}))

    def collect(dst, send, recv):
        for d in range(1, 8):
            peer = lax.rem(v + d, 8)
            remote(dst.at[peer], dst.at[peer], send.at[peer], recv.at[peer], {"vid": peer}).wait_recv()

    close = [(0, 1), (1, 0), (3, 0), (1, 1), (3, 1)]
    distant = [(2, 0), (2, 1)]

    factor = 128 ** (-0.5)

    def attention(net, m, save):
        for h in range(2):
            queries = QR[net, m, :, 128 * h : 128 * h + 128]
            keys = KV[net, :, :, :, 256 * h : 256 * h + 128].reshape(768, 128)
            values = KV[net, :, :, :, 256 * h + 128 : 256 * h + 256].reshape(768, 128)
            scores = dot(queries, keys, NT) * factor + BIAS[m]
            shifted = jnp.exp(scores - jnp.max(scores, -1, keepdims=True))
            prob = shifted * (1.0 / jnp.sum(shifted, -1, keepdims=True))
            if save:
                PS[2 * m + h] = prob
            OB[net, m, :, 128 * h : 128 * h + 128] = dot(prob.astype(BF16), values, NN).astype(BF16)

    def project_out(net, m):
        return dot(OB[net, m], WO[m], NN)

    def aud(i, g, m, kind, src, dst, device):
        return remote(src, dst, ar_s.at[i, g, m, kind], ar_r.at[i, g, m, kind], {"aud": device})

    def sum_start(i, m):
        for kind, part in ((0, give), (1, hold)):
            for g in range(2):
                go(aud(i, g, m, kind, SB.at[i, m, part[g, m]], R1.at[i, g, m, kind], first[m]))

    def sum_1(i):
        for g, m in chunks:
            aud(i, g, m, 0, R1.at[i, g, m, 0], R1.at[i, g, m, 0], first[m]).wait_recv()
            S2[i, g, m] = (wide(SB[i, m, other[g, m], :]) + wide(R1[i, g, m, 0])).astype(BF16)
            go(aud(i, g, m, 2, S2.at[i, g, m], R2.at[i, g, m], second[m]))

    def sum_2(i):
        for g, m in chunks:
            aud(i, g, m, 1, R1.at[i, g, m, 1], R1.at[i, g, m, 1], first[m]).wait_recv()
            aud(i, g, m, 2, R2.at[i, g, m], R2.at[i, g, m], second[m]).wait_recv()
            ZS[i, g, m] = (
                wide(SB[i, m, own[g, m], :]) + wide(R1[i, g, m, 1]) + wide(R2[i, g, m])
            ).astype(BF16)
            go(aud(i, g, m, 3, ZS.at[i, g, m], ZR.at[i, g, m], across))

    def summed(i, g, m):
        aud(i, g, m, 3, ZR.at[i, g, m], ZR.at[i, g, m], across).wait_recv()
        return wide(ZS[i, g, m]) + wide(ZR[i, g, m])

    def share(i, g, m, value):
        AG[i, m, own[g, m], :] = value.astype(BF16)
        part = AG.at[i, m, own[g, m]]
        go(aud(i, g, m, 4, part, part, second[m]))
        go(aud(i, g, m, 5, part, part, first[m]))

    def share_on(i):
        for g, m in chunks:
            part = AG.at[i, m, other[g, m]]
            aud(i, g, m, 4, part, part, second[m]).wait_recv()
            go(aud(i, g, m, 6, part, part, first[m]))

    def share_end(i):
        for g, m in chunks:
            part = AG.at[i, m, hold[g, m]]
            aud(i, g, m, 5, part, part, first[m]).wait_recv()
            part = AG.at[i, m, give[g, m]]
            aud(i, g, m, 6, part, part, first[m]).wait_recv()

    for m in range(2):
        loads[2 + m].wait()
    kv_wait(T1)
    for m in range(2):
        attention(T1, m, False)
        field = project_out(T1, m)
        SB[0, m] = field.astype(BF16)
        ACC[m] = -field
        sum_start(0, m)
    kv_wait(ST)
    NG[v] = NS[core, :, yy]
    spread(lambda k, y: NS.at[k, :, y], NG, ng_s, ng_r, close + distant)
    attention(ST, 0, True)
    sum_1(0)
    attention(ST, 1, True)
    OG[v] = OB[ST, core]
    spread(lambda k, y: OB.at[ST, k], OG, og_s, og_r, close + distant)
    sum_2(0)
    for m in range(2):
        ACC[m] = ACC[m] + 2.0 * project_out(ST, m)
    for g, m in chunks:
        cur = wide(xs[m][own[g, m], :]) + step * summed(0, g, m)
        inv = lax.rsqrt(jnp.mean(cur * cur, -1, keepdims=True) + EPSILON)
        share(0, g, m, cur * inv * MODS[4 + m : 5 + m, :])
    share_on(0)
    share_end(0)

    for m in range(2):
        store_qkv(T2, m, dot(AG[0, m], WQ[m], NN))
    kv_start(T2)
    kv_wait(T2)
    for m in range(2):
        attention(T2, m, False)
        SB[1, m] = (ACC[m] - project_out(T2, m)).astype(BF16)
        sum_start(1, m)
    collect(NG, ng_s, ng_r)
    for s in range(4):
        NGT[128 * s : 128 * s + 128, :] = NG[:, s].reshape(1024, 128).T
    sum_1(1)
    collect(OG, og_s, og_r)
    sum_2(1)
    for g, m in chunks:
        diff = step * summed(1, g, m)
        DIFF[g, m] = diff
        share(1, g, m, 2.0 * step * diff)
    share_on(1)
    share_end(1)

    for m in range(2):
        for s in range(16):
            GS[m, s // 4, s % 4] = AG[1, m, :, 128 * s : 128 * s + 128]
    GG[v] = GS[core, :, yy]
    spread(lambda k, y: GS.at[k, :, y], GG, gg_s, gg_r, close)
    for m in range(2):
        DO[m] = dot(AG[1, m], WO[m], NT).astype(BF16)
    for m in range(2):
        for h in range(2):
            cols = slice(256 * h, 256 * h + 128)
            vcols = slice(256 * h + 128, 256 * h + 256)
            queries = QR[ST, m, :, 128 * h : 128 * h + 128]
            keys = KV[ST, :, :, :, cols].reshape(768, 128)
            values = KV[ST, :, :, :, vcols].reshape(768, 128)
            grad_out = DO[m, :, 128 * h : 128 * h + 128]
            prob = PS[2 * m + h]
            grad_prob = dot(grad_out, values, NT)
            center = jnp.sum(prob * grad_prob, -1, keepdims=True)
            dscore = (prob * (grad_prob - center) * factor).astype(BF16)
            dquery = dot(dscore, keys, NN).astype(BF16)
            DQ[m, :, 384 * h : 384 * h + 128] = dquery
            DQS[0, m, :, 128 * h : 128 * h + 128] = dquery
            dkey = dot(dscore, queries, TN).reshape(3, 2, 128, 128)
            dvalue = dot(prob.astype(BF16), grad_out, TN).reshape(3, 2, 128, 128)
            if m == 0:
                DKV[:, :, :, cols] = dkey
                DKV[:, :, :, vcols] = dvalue
            else:
                DKV[:, :, :, cols] = DKV[:, :, :, cols] + dkey
                DKV[:, :, :, vcols] = DKV[:, :, :, vcols] + dvalue
    DKS[0] = DKV[0].astype(BF16)
    DKS[1] = DKV[2].astype(BF16)
    edges = (
        remote(DKS.at[0], DKR.at[0], kv_s.at[6], kv_r.at[6], {"vid": left}),
        remote(DKS.at[1], DKR.at[1], kv_s.at[7], kv_r.at[7], {"vid": right}),
    )
    for copy in edges:
        go(copy)

    def line(n, k, part, device):
        return remote(part, part, dg_s.at[n, k], dg_r.at[n, k], {"vid": device})

    def line_start(n):
        DG[n, yy, core] = DQS[n, core]
        go(remote(DQS.at[n, 1 - core], DG.at[n, yy, core], dg_s.at[n, 0], dg_r.at[n, 0], {"vid": mate}))

    def line_send(n):
        line(n, 0, DG.at[n, yy, 1 - core], mate).wait_recv()
        go(line(n, 1, DG.at[n, yy], 2 * y_one + core))
        go(line(n, 2, DG.at[n, yy], 2 * y_two + core))

    def line_on(n):
        line(n, 1, DG.at[n, y_one], 2 * y_one + core).wait_recv()
        go(line(n, 3, DG.at[n, y_one], 2 * y_two + core))

    def line_end(n):
        line(n, 2, DG.at[n, y_two], 2 * y_two + core).wait_recv()
        line(n, 3, DG.at[n, y_last], 2 * y_two + core).wait_recv()

    line_start(0)
    line_send(0)
    for copy in edges:
        copy.wait_recv()
    for m in range(2):
        owned = (DKV[1, m] + wide(DKR[0, m]) + wide(DKR[1, m])).astype(BF16)
        for h in range(2):
            DQS[1 + h, m] = owned[:, 256 * h : 256 * h + 256]
            DQ[m, :, 384 * h + 128 : 384 * h + 384] = owned[:, 256 * h : 256 * h + 256]
    line_start(1)
    line_start(2)
    SB[2, 0] = dot(DQ[0], WQ[0], NT).astype(BF16)
    sum_start(2, 0)
    line_send(1)
    line_send(2)
    SB[2, 1] = dot(DQ[1], WQ[1], NT).astype(BF16)
    sum_start(2, 1)
    line_on(0)

    c_one = c + 1 - 2 * lax.rem(c, 2)
    c_two = lax.rem(c + 2, 4)
    c_not = lax.rem(c_one + 2, 4)
    mine = pl.ds(pl.multiple_of(64 * core, 64), 64)
    theirs = pl.ds(pl.multiple_of(64 * (1 - core), 64), 64)

    def clip_start(n):
        for k, block in ((0, c_one), (1, c_not)):
            go(remote(W.at[n, block], WR.at[n, k], cl_s.at[n, k], cl_r.at[n, k], {"clip": c_one}))

    def clip_on(n):
        for k, block in ((1, c_two), (0, c)):
            part = WR.at[n, k]
            remote(part, part, cl_s.at[n, k], cl_r.at[n, k], {"clip": c_one}).wait_recv()
            WS[n, k] = (wide(W[n, block]) + wide(WR[n, k])).astype(BF16)
            if k == 1:
                for j, half, device in ((2, mine, {"clip": c_two}), (3, theirs, {"clip": c_two, "vid": mate})):
                    go(remote(WS.at[n, 1, half], WF.at[n, core, 1], cl_s.at[n, j], wf_r.at[n, core, 1], device))
            else:
                go(remote(WS.at[n, 0, theirs], WF.at[n, core, 0], cl_s.at[n, 4], wf_r.at[n, core, 0], {"vid": mate}))
                WF[n, core, 0] = WS[n, 0, mine, :]

    def clip_end(n):
        for src, k, device in (
            (core, 1, {"clip": c_two}), (1 - core, 1, {"clip": c_two, "vid": mate}), (1 - core, 0, {"vid": mate})
        ):
            part = WF.at[n, src, k]
            remote(part, part, cl_s.at[n, 2], wf_r.at[n, src, k], device).wait_recv()
        return [wide(WF[n, m, 0]) + wide(WF[n, m, 1]) for m in range(2)]

    def line_grad(n):
        line_end(n)
        W[n] = dot(NGT[...], DG[n].reshape(1024, 256), NN).astype(BF16).reshape(4, 128, 256)
        clip_start(n)

    sum_1(2)
    line_on(1)
    line_grad(0)
    sum_2(2)
    line_on(2)
    line_grad(1)
    spread(lambda k, y: GS.at[k, :, y], GG, gg_s, gg_r, distant)
    clip_on(0)
    line_grad(2)
    for g, m in chunks:
        cur = wide(xs[m][own[g, m], :])
        inv = lax.rsqrt(jnp.mean(cur * cur, -1, keepdims=True) + EPSILON)
        scaled = summed(2, g, m) * MODS[2 + m : 3 + m, :]
        back = inv * scaled - cur * (inv * inv * inv) * jnp.mean(scaled * cur, -1, keepdims=True)
        share(2, g, m, DIFF[g, m] + back)
    clip_on(1)
    collect(GG, gg_s, gg_r)
    o_all = OG[...].reshape(1024, 256)
    for s in range(4):
        W[3, s] = dot(GG[:, s].reshape(1024, 128), o_all, TN).astype(BF16)
    clip_start(3)
    share_on(2)
    clip_on(2)
    clip_on(3)
    q_outs = (qv_out, qa_out)
    o_outs = (ov_out, oa_out)
    for m, total in enumerate(clip_end(0)):
        for h in range(2):
            q_outs[m][:, h, 0:128] = total[:, 128 * h : 128 * h + 128]
    for h in range(2):
        if h == 1:
            share_end(2)
            outs = (
                pltpu.make_async_copy(AG.at[2, 0], dv_out, o_sem.at[0]),
                pltpu.make_async_copy(AG.at[2, 1], da_out, o_sem.at[1]),
            )
            for copy in outs:
                copy.start()
        for m, total in enumerate(clip_end(1 + h)):
            q_outs[m][:, h, 128:384] = total
    for m, total in enumerate(clip_end(3)):
        for h in range(2):
            o_outs[m][h] = total[:, 128 * h : 128 * h + 128]
    for copy in outs:
        copy.wait()
    for copy in pending:
        copy.wait_send()


def vm(shape, kind=BF16):
    return pltpu.VMEM(shape, kind)


def fused(*operands):
    dma = pltpu.SemaphoreType.DMA
    inside = pl.BlockSpec(memory_space=pltpu.VMEM)
    scalar = pl.BlockSpec(memory_space=pltpu.SMEM)
    outside = pl.BlockSpec(memory_space=pl.ANY)
    shape = jax.ShapeDtypeStruct
    return pl.pallas_call(
        kernel,
        out_shape=(
            shape((128, 2048), BF16), shape((128, 2048), BF16), shape((64, 2, 384), F32),
            shape((64, 2, 384), F32), shape((2, 64, 128), F32), shape((2, 64, 128), F32),
        ),
        in_specs=[scalar] * 3 + [inside] * 6 + [outside] * 4,
        out_specs=(outside, outside, inside, inside, inside, inside),
        scratch_shapes=[
            vm((2, 2048, 768)), vm((2, 256, 2048)), vm((2, 2, 128, 2048)), vm((2, 4, 4, 128, 128)),
            vm((8, 4, 128, 128)), vm((512, 1024)), vm((3, 2, 128, 256)), vm((8, 128, 256)),
            vm((2, 4, 4, 128, 128)), vm((8, 4, 128, 128)), vm((2, 128, 768)), vm((3, 2, 128, 256)),
            vm((3, 4, 2, 128, 256)), vm((3, 2, 128, 256)),
            vm((3, 3, 2, 128, 512)), vm((4, 128, 768), F32), vm((2, 128, 2048), F32),
            vm((3, 2, 128, 2048)), vm((3, 2, 2, 2, 16, 2048)), vm((3, 2, 2, 16, 2048)),
            vm((3, 2, 2, 16, 2048)), vm((3, 2, 2, 16, 2048)), vm((3, 2, 2, 16, 2048)),
            vm((3, 2, 128, 2048)), vm((2, 2, 16, 2048), F32), vm((2, 128, 256)),
            vm((3, 2, 128, 512), F32), vm((2, 2, 128, 512)), vm((2, 2, 128, 512)),
            vm((4, 4, 128, 256)), vm((4, 2, 128, 256)), vm((4, 2, 128, 256)), vm((4, 2, 2, 64, 256)),
            vm((8, 2048), F32), vm((2, 128, 768), F32),
            dma((4,)), dma((2,)), dma((8,)), dma((8,)), dma((3, 2, 2, 7)), dma((3, 2, 2, 7)),
            dma((8,)), dma((8,)), dma((8,)), dma((8,)), dma((8,)), dma((8,)),
            dma((3, 4)), dma((3, 4)), dma((4, 5)), dma((4, 2)), dma((4, 2, 2)),
        ],
        compiler_params=pltpu.CompilerParams(
            collective_id=0, has_side_effects=True, vmem_limit_bytes=VMEM_LIMIT
        ),
        name="step",
    )(*operands)


def finish_kernel(*refs):
    for src, dst in zip(refs[:6], refs[6:]):
        dst[...] = src[...]


def finish(*results):
    inside = pl.BlockSpec(memory_space=pltpu.VMEM)
    return pl.pallas_call(
        finish_kernel,
        out_shape=tuple(jax.ShapeDtypeStruct(r.shape, r.dtype) for r in results),
        in_specs=[inside] * 6,
        out_specs=(inside,) * 6,
        compiler_params=pltpu.CompilerParams(vmem_limit_bytes=8 * 1024 * 1024),
        name="finish",
    )(*results)


def local(
    video_tokens, audio_tokens, qkv_video, out_video, qkv_audio, out_audio, gain_video, gain_audio,
    time_from, time_to, time_steps, windows, intersection,
):
    d_video, d_audio, qv, qa, ov, oa = finish(*fused(
        time_steps, windows, intersection.swapaxes(1, 2), video_tokens[0], audio_tokens[0],
        gain_video.reshape(1, 2048), gain_audio.reshape(1, 2048), time_from, time_to,
        qkv_video.reshape(2048, 768), qkv_audio.reshape(2048, 768),
        out_video.reshape(256, 2048), out_audio.reshape(256, 2048),
    ))
    return d_video[None], d_audio[None], qv, ov.swapaxes(1, 2), qa, oa.swapaxes(1, 2)


def solution(mesh):
    return jax.shard_map(
        local,
        mesh=mesh,
        in_specs=(
            P("clip", "vid", None), P("clip", "vid", None), P(None, "aud", None), P("aud", None, None),
            P(None, "aud", None), P("aud", None, None), P(), P(), P(), P(),
            P("clip", None), P("clip", None), P("clip", None, None),
        ),
        out_specs=(
            P("clip", "vid", None), P("clip", "vid", None), P(("clip", "vid"), "aud", None),
            P("aud", None, ("clip", "vid")), P(("clip", "vid"), "aud", None), P("aud", None, ("clip", "vid")),
        ),
        check_vma=False,
    )
```

```python
import jax
import jax.numpy as jnp
from jax import lax
from jax.experimental import pallas as pl
from jax.experimental.pallas import tpu as pltpu
from jax.sharding import PartitionSpec as P

BLK = 32
TGRID = 64
STEPS = 2
EPSILON = 1e-06
MESH = pl.DeviceIdType.MESH
F32 = jnp.float32
BF16 = jnp.bfloat16
NT = (((1,), (1,)), ((), ()))
TN = (((0,), (0,)), ((), ()))
NN = (((1,), (0,)), ((), ()))
T1, ST, T2 = 0, 1, 2
VMEM_LIMIT = 42 * 1024 * 1024


def dot(a, b, dims):
    return lax.dot_general(a, b, dims, preferred_element_type=F32)


def kernel(
    steps, windows, ranges, xv, xa, gv, ga, tf, tt, wqv, wqa, wov, woa,
    dv_out, da_out, qv_out, qa_out, ov_out, oa_out,
    N0, NS, NG, NGT, OB, OG, GS, GG, DQ, DQS, DG, QR, KV, PS, ACC,
    SB, R1, S2, R2, ZS, ZR, AG, DIFF, DO, DKV, DKS, DKR,
    W, WR, WS, WF, MODS, BIAS,
    kv_s, kv_r, ar_s, ar_r, ng_s, ng_r, og_s, og_r, gg_s, gg_r,
    dg_s, dg_r, cl_s, cl_r, wf_r,
):
    v = lax.axis_index("vid")
    a = lax.axis_index("aud")
    c = lax.axis_index("clip")
    core = lax.rem(v, 2)
    yy = v // 2
    x = a // 2
    zh = lax.rem(a, 2)
    b0 = lax.rem(x, 2)
    b1 = x // 2
    q = lax.rem(b0 + b1, 2)
    near = (x + 1 - 2 * b0) * 2 + zh
    far = (3 - x) * 2 + zh
    across = a + 1 - 2 * zh
    first = (near, far)
    second = (far, near)
    keep1 = (q, b1)
    keep2 = (b1, b0)
    keepf = (b1, 1 - b0)
    right = lax.rem(v + 1, 8)
    left = lax.rem(v + 7, 8)
    y_near = yy + 1 - 2 * lax.rem(yy, 2)
    y_far = 3 - yy
    y_one = (1 - core) * y_near + core * y_far
    y_two = core * y_near + (1 - core) * y_far
    y_last = 6 - yy - y_one - y_two
    mate = v + 1 - 2 * core

    def rows(value):
        return pl.ds(pl.multiple_of(value, 16), 16)

    chunks = [(g, m) for g in range(2) for m in range(2)]
    own, other, give, hold = {}, {}, {}, {}
    for g, m in chunks:
        base = 64 * g + 32 * keep1[m]
        away = 64 * g + 32 * (1 - keep1[m])
        own[g, m] = rows(base + 16 * keep2[m])
        other[g, m] = rows(base + 16 * (1 - keep2[m]))
        give[g, m] = rows(away + 16 * (1 - keepf[m]))
        hold[g, m] = rows(away + 16 * keepf[m])

    barrier = pltpu.get_barrier_semaphore()
    greet = [{"vid": lax.rem(v + d, 8)} for d in range(1, 8)]
    greet += [{"aud": peer} for peer in (near, far, across)]
    greet += [{"clip": c + 1 - 2 * lax.rem(c, 2)}]
    greet += [{"clip": lax.rem(c + 2, 4), "vid": 2 * yy + k} for k in range(2)]
    for peer in greet:
        pl.semaphore_signal(barrier, 1, device_id=peer, device_id_type=MESH)

    WQ = (wqv, wqa)
    WO = (wov, woa)
    pending = []

    def remote(src, dst, send, recv, device):
        return pltpu.make_async_remote_copy(
            src_ref=src, dst_ref=dst, send_sem=send, recv_sem=recv, device_id=device, device_id_type=MESH
        )

    def go(copy):
        copy.start()
        pending.append(copy)

    def wide(ref):
        return ref.astype(F32)

    now = steps[0, 0]
    stride = steps[0, 1]
    step = -stride.astype(F32) / TGRID
    conds = (
        tf[pl.ds(now, 1), :] + tt[pl.ds(now, 1), :],
        tf[pl.ds(now, 1), :] + tt[pl.ds(now - STEPS * stride, 1), :],
        tf[pl.ds(now - stride, 1), :] + tt[pl.ds(now - stride, 1), :],
    )
    gains = (gv, ga)
    for net in range(3):
        for m in range(2):
            MODS[2 * net + m : 2 * net + m + 1, :] = gains[m][...] * (1.0 + conds[net])

    xs = (xv, xa)

    def normed(net, m, r):
        part = pl.ds(pl.multiple_of(r * 32, 32), 32)
        cur = wide(xs[m][part, :])
        inv = lax.rsqrt(jnp.mean(cur * cur, -1, keepdims=True) + EPSILON)
        out = (cur * inv * MODS[2 * net + m : 2 * net + m + 1, :]).astype(BF16)
        N0[net, m, part, :] = out
        return part, out

    def store_qkv(net, m, value):
        rounded = value.astype(BF16)
        for h in range(2):
            QR[net, m, :, 128 * h : 128 * h + 128] = rounded[:, 384 * h : 384 * h + 128]
            KV[net, 1, m, :, 256 * h : 256 * h + 256] = rounded[:, 384 * h + 128 : 384 * h + 384]

    def kv_copies(net):
        return (
            remote(KV.at[net, 1], KV.at[net, 0], kv_s.at[2 * net], kv_r.at[2 * net], {"vid": right}),
            remote(KV.at[net, 1], KV.at[net, 2], kv_s.at[2 * net + 1], kv_r.at[2 * net + 1], {"vid": left}),
        )

    def kv_start(net):
        for copy in kv_copies(net):
            go(copy)

    def kv_wait(net):
        for copy in kv_copies(net):
            copy.wait_recv()

    for m in range(2):

        def norm_teacher(r, carry, m=m):
            normed(T1, m, r)
            return carry

        lax.fori_loop(0, 4, norm_teacher, 0)
    for m in range(2):
        store_qkv(T1, m, dot(N0[T1, m], WQ[m][...], NN))
    pl.semaphore_wait(barrier, len(greet))
    kv_start(T1)

    for m in range(2):

        def norm_student(r, carry, m=m):
            part, student = normed(ST, m, r)
            for s in range(16):
                NS[m, s // 4, s % 4, part, :] = student[:, 128 * s : 128 * s + 128]
            return carry

        lax.fori_loop(0, 4, norm_student, 0)
        store_qkv(ST, m, dot(N0[ST, m], WQ[m][...], NN))
    kv_start(ST)

    qpos = lax.broadcasted_iota(jnp.int32, (128, 128), 0)
    kpos = lax.broadcasted_iota(jnp.int32, (128, 128), 1)
    qblk = lax.broadcasted_iota(jnp.int32, (128, 1), 0) // BLK
    kblk = lax.broadcasted_iota(jnp.int32, (1, 128), 1) // BLK

    def spans(which, first_block, block_of):
        out = jnp.zeros(block_of.shape, jnp.int32)
        for i in range(4):
            at = jnp.clip(first_block + i, 0, 31)
            out = jnp.where(block_of == i, ranges[0, which, at], out)
        return out

    low_q = spans(0, 4 * v, qblk)
    high_q = spans(1, 4 * v, qblk)
    for slot in range(3):
        shard = v + slot - 1
        at = kpos + 128 * shard
        inside = (at >= 0) & (at < 1024)
        apart = jnp.abs(qpos - (kpos + 128 * (slot - 1)))
        keys_at = kblk + 4 * shard
        low_k = spans(0, 4 * shard, kblk)
        high_k = spans(1, 4 * shard, kblk)
        query_at = qblk + 4 * v
        tests = (
            (apart < windows[0, 0], (keys_at >= low_q) & (keys_at < high_q)),
            ((query_at >= low_k) & (query_at < high_k), apart < windows[0, 1]),
        )
        for m in range(2):
            for k in range(2):
                cols = slice(256 * slot + 128 * k, 256 * slot + 128 * k + 128)
                BIAS[m, :, cols] = jnp.where(inside & tests[m][k], 0.0, -1e30)

    def spread(src, dst, send, recv, offsets):
        for d in offsets:
            peer = 2 * lax.rem(yy + d[0], 4) + lax.rem(core + d[1], 2)
            go(remote(src(lax.rem(peer, 2), peer // 2), dst.at[v], send.at[peer], recv.at[v], {"vid": peer}))

    def collect(dst, send, recv):
        for d in range(1, 8):
            peer = lax.rem(v + d, 8)
            remote(dst.at[peer], dst.at[peer], send.at[peer], recv.at[peer], {"vid": peer}).wait_recv()

    close = [(0, 1), (1, 0), (3, 0), (1, 1), (3, 1)]
    distant = [(2, 0), (2, 1)]

    factor = 128 ** (-0.5)

    def attention(net, m, save):
        for h in range(2):
            queries = QR[net, m, :, 128 * h : 128 * h + 128]
            keys = KV[net, :, :, :, 256 * h : 256 * h + 128].reshape(768, 128)
            values = KV[net, :, :, :, 256 * h + 128 : 256 * h + 256].reshape(768, 128)
            scores = dot(queries, keys, NT) * factor + BIAS[m]
            shifted = jnp.exp(scores - jnp.max(scores, -1, keepdims=True))
            prob = shifted * (1.0 / jnp.sum(shifted, -1, keepdims=True))
            if save:
                PS[2 * m + h] = prob
            OB[net, m, :, 128 * h : 128 * h + 128] = dot(prob.astype(BF16), values, NN).astype(BF16)

    def project_out(net, m):
        return dot(OB[net, m], WO[m][...], NN)

    def aud(i, g, m, kind, src, dst, device):
        return remote(src, dst, ar_s.at[i, g, m, kind], ar_r.at[i, g, m, kind], {"aud": device})

    def sum_start(i, m):
        for kind, part in ((0, give), (1, hold)):
            for g in range(2):
                go(aud(i, g, m, kind, SB.at[i, m, part[g, m]], R1.at[i, g, m, kind], first[m]))

    def sum_1(i):
        for g, m in chunks:
            aud(i, g, m, 0, R1.at[i, g, m, 0], R1.at[i, g, m, 0], first[m]).wait_recv()
            S2[i, g, m] = (wide(SB[i, m, other[g, m], :]) + wide(R1[i, g, m, 0])).astype(BF16)
            go(aud(i, g, m, 2, S2.at[i, g, m], R2.at[i, g, m], second[m]))

    def sum_2(i):
        for g, m in chunks:
            aud(i, g, m, 1, R1.at[i, g, m, 1], R1.at[i, g, m, 1], first[m]).wait_recv()
            aud(i, g, m, 2, R2.at[i, g, m], R2.at[i, g, m], second[m]).wait_recv()
            ZS[i, g, m] = (
                wide(SB[i, m, own[g, m], :]) + wide(R1[i, g, m, 1]) + wide(R2[i, g, m])
            ).astype(BF16)
            go(aud(i, g, m, 3, ZS.at[i, g, m], ZR.at[i, g, m], across))

    def summed(i, g, m):
        aud(i, g, m, 3, ZR.at[i, g, m], ZR.at[i, g, m], across).wait_recv()
        return wide(ZS[i, g, m]) + wide(ZR[i, g, m])

    def share(i, g, m, value):
        AG[i, m, own[g, m], :] = value.astype(BF16)
        part = AG.at[i, m, own[g, m]]
        go(aud(i, g, m, 4, part, part, second[m]))
        go(aud(i, g, m, 5, part, part, first[m]))

    def share_on(i):
        for g, m in chunks:
            part = AG.at[i, m, other[g, m]]
            aud(i, g, m, 4, part, part, second[m]).wait_recv()
            go(aud(i, g, m, 6, part, part, first[m]))

    def share_end(i):
        for g, m in chunks:
            part = AG.at[i, m, hold[g, m]]
            aud(i, g, m, 5, part, part, first[m]).wait_recv()
            part = AG.at[i, m, give[g, m]]
            aud(i, g, m, 6, part, part, first[m]).wait_recv()

    kv_wait(T1)
    for m in range(2):
        attention(T1, m, False)
        field = project_out(T1, m)
        SB[0, m] = field.astype(BF16)
        ACC[m] = -field
        sum_start(0, m)
    kv_wait(ST)
    NG[v] = NS[core, :, yy]
    spread(lambda k, y: NS.at[k, :, y], NG, ng_s, ng_r, close + distant)
    attention(ST, 0, True)
    sum_1(0)
    attention(ST, 1, True)
    OG[v] = OB[ST, core]
    spread(lambda k, y: OB.at[ST, k], OG, og_s, og_r, close + distant)
    sum_2(0)
    for m in range(2):
        ACC[m] = ACC[m] + 2.0 * project_out(ST, m)
    for g, m in chunks:
        cur = wide(xs[m][own[g, m], :]) + step * summed(0, g, m)
        inv = lax.rsqrt(jnp.mean(cur * cur, -1, keepdims=True) + EPSILON)
        share(0, g, m, cur * inv * MODS[4 + m : 5 + m, :])
    share_on(0)
    share_end(0)

    for m in range(2):
        store_qkv(T2, m, dot(AG[0, m], WQ[m][...], NN))
    kv_start(T2)
    kv_wait(T2)
    for m in range(2):
        attention(T2, m, False)
        SB[1, m] = (ACC[m] - project_out(T2, m)).astype(BF16)
        sum_start(1, m)
    collect(NG, ng_s, ng_r)
    for s in range(4):
        NGT[128 * s : 128 * s + 128, :] = NG[:, s].reshape(1024, 128).T
    sum_1(1)
    collect(OG, og_s, og_r)
    sum_2(1)
    for g, m in chunks:
        diff = step * summed(1, g, m)
        DIFF[g, m] = diff
        share(1, g, m, 2.0 * step * diff)
    share_on(1)
    share_end(1)

    for m in range(2):
        for s in range(16):
            GS[m, s // 4, s % 4] = AG[1, m, :, 128 * s : 128 * s + 128]
    GG[v] = GS[core, :, yy]
    spread(lambda k, y: GS.at[k, :, y], GG, gg_s, gg_r, close)
    for m in range(2):
        DO[m] = dot(AG[1, m], WO[m][...], NT).astype(BF16)
    for m in range(2):
        for h in range(2):
            cols = slice(256 * h, 256 * h + 128)
            vcols = slice(256 * h + 128, 256 * h + 256)
            queries = QR[ST, m, :, 128 * h : 128 * h + 128]
            keys = KV[ST, :, :, :, cols].reshape(768, 128)
            values = KV[ST, :, :, :, vcols].reshape(768, 128)
            grad_out = DO[m, :, 128 * h : 128 * h + 128]
            prob = PS[2 * m + h]
            grad_prob = dot(grad_out, values, NT)
            center = jnp.sum(prob * grad_prob, -1, keepdims=True)
            dscore = (prob * (grad_prob - center) * factor).astype(BF16)
            dquery = dot(dscore, keys, NN).astype(BF16)
            DQ[m, :, 384 * h : 384 * h + 128] = dquery
            DQS[0, m, :, 128 * h : 128 * h + 128] = dquery
            dkey = dot(dscore, queries, TN).reshape(3, 2, 128, 128)
            dvalue = dot(prob.astype(BF16), grad_out, TN).reshape(3, 2, 128, 128)
            if m == 0:
                DKV[:, :, :, cols] = dkey
                DKV[:, :, :, vcols] = dvalue
            else:
                DKV[:, :, :, cols] = DKV[:, :, :, cols] + dkey
                DKV[:, :, :, vcols] = DKV[:, :, :, vcols] + dvalue
    DKS[0] = DKV[0].astype(BF16)
    DKS[1] = DKV[2].astype(BF16)
    edges = (
        remote(DKS.at[0], DKR.at[0], kv_s.at[6], kv_r.at[6], {"vid": left}),
        remote(DKS.at[1], DKR.at[1], kv_s.at[7], kv_r.at[7], {"vid": right}),
    )
    for copy in edges:
        go(copy)

    def line(n, k, part, device):
        return remote(part, part, dg_s.at[n, k], dg_r.at[n, k], {"vid": device})

    def line_start(n):
        DG[n, yy, core] = DQS[n, core]
        go(remote(DQS.at[n, 1 - core], DG.at[n, yy, core], dg_s.at[n, 0], dg_r.at[n, 0], {"vid": mate}))

    def line_send(n):
        line(n, 0, DG.at[n, yy, 1 - core], mate).wait_recv()
        go(line(n, 1, DG.at[n, yy], 2 * y_one + core))
        go(line(n, 2, DG.at[n, yy], 2 * y_two + core))

    def line_on(n):
        line(n, 1, DG.at[n, y_one], 2 * y_one + core).wait_recv()
        go(line(n, 3, DG.at[n, y_one], 2 * y_two + core))

    def line_end(n):
        line(n, 2, DG.at[n, y_two], 2 * y_two + core).wait_recv()
        line(n, 3, DG.at[n, y_last], 2 * y_two + core).wait_recv()

    line_start(0)
    line_send(0)
    for copy in edges:
        copy.wait_recv()
    for m in range(2):
        owned = (DKV[1, m] + wide(DKR[0, m]) + wide(DKR[1, m])).astype(BF16)
        for h in range(2):
            DQS[1 + h, m] = owned[:, 256 * h : 256 * h + 256]
            DQ[m, :, 384 * h + 128 : 384 * h + 384] = owned[:, 256 * h : 256 * h + 256]
    line_start(1)
    line_start(2)
    SB[2, 0] = dot(DQ[0], WQ[0][...], NT).astype(BF16)
    sum_start(2, 0)
    line_send(1)
    line_send(2)
    SB[2, 1] = dot(DQ[1], WQ[1][...], NT).astype(BF16)
    sum_start(2, 1)
    line_on(0)

    c_one = c + 1 - 2 * lax.rem(c, 2)
    c_two = lax.rem(c + 2, 4)
    c_not = lax.rem(c_one + 2, 4)
    mine = pl.ds(pl.multiple_of(64 * core, 64), 64)
    theirs = pl.ds(pl.multiple_of(64 * (1 - core), 64), 64)

    def clip_start(n):
        for k, block in ((0, c_one), (1, c_not)):
            go(remote(W.at[n, block], WR.at[n, k], cl_s.at[n, k], cl_r.at[n, k], {"clip": c_one}))

    def clip_on(n):
        for k, block in ((1, c_two), (0, c)):
            part = WR.at[n, k]
            remote(part, part, cl_s.at[n, k], cl_r.at[n, k], {"clip": c_one}).wait_recv()
            WS[n, k] = (wide(W[n, block]) + wide(WR[n, k])).astype(BF16)
            if k == 1:
                for j, half, device in ((2, mine, {"clip": c_two}), (3, theirs, {"clip": c_two, "vid": mate})):
                    go(remote(WS.at[n, 1, half], WF.at[n, core, 1], cl_s.at[n, j], wf_r.at[n, core, 1], device))
            else:
                go(remote(WS.at[n, 0, theirs], WF.at[n, core, 0], cl_s.at[n, 4], wf_r.at[n, core, 0], {"vid": mate}))
                WF[n, core, 0] = WS[n, 0, mine, :]

    def clip_end(n):
        for src, k, device in (
            (core, 1, {"clip": c_two}), (1 - core, 1, {"clip": c_two, "vid": mate}), (1 - core, 0, {"vid": mate})
        ):
            part = WF.at[n, src, k]
            remote(part, part, cl_s.at[n, 2], wf_r.at[n, src, k], device).wait_recv()
        return [wide(WF[n, m, 0]) + wide(WF[n, m, 1]) for m in range(2)]

    def line_grad(n):
        line_end(n)
        W[n] = dot(NGT[...], DG[n].reshape(1024, 256), NN).astype(BF16).reshape(4, 128, 256)
        clip_start(n)

    sum_1(2)
    line_on(1)
    line_grad(0)
    sum_2(2)
    line_on(2)
    line_grad(1)
    spread(lambda k, y: GS.at[k, :, y], GG, gg_s, gg_r, distant)
    clip_on(0)
    line_grad(2)
    for g, m in chunks:
        cur = wide(xs[m][own[g, m], :])
        inv = lax.rsqrt(jnp.mean(cur * cur, -1, keepdims=True) + EPSILON)
        scaled = summed(2, g, m) * MODS[2 + m : 3 + m, :]
        back = inv * scaled - cur * (inv * inv * inv) * jnp.mean(scaled * cur, -1, keepdims=True)
        share(2, g, m, DIFF[g, m] + back)
    clip_on(1)
    collect(GG, gg_s, gg_r)
    o_all = OG[...].reshape(1024, 256)
    for s in range(4):
        W[3, s] = dot(GG[:, s].reshape(1024, 128), o_all, TN).astype(BF16)
    clip_start(3)
    share_on(2)
    clip_on(2)
    clip_on(3)
    q_outs = (qv_out, qa_out)
    o_outs = (ov_out, oa_out)
    for m, total in enumerate(clip_end(0)):
        for h in range(2):
            q_outs[m][:, h, 0:128] = total[:, 128 * h : 128 * h + 128]
    for h in range(2):
        if h == 1:
            share_end(2)
            dv_out[...] = AG[2, 0]
            da_out[...] = AG[2, 1]
        for m, total in enumerate(clip_end(1 + h)):
            q_outs[m][:, h, 128:384] = total
    for m, total in enumerate(clip_end(3)):
        for h in range(2):
            o_outs[m][h] = total[:, 128 * h : 128 * h + 128]
    for copy in pending:
        copy.wait_send()


def vm(shape, kind=BF16):
    return pltpu.VMEM(shape, kind)


def fused(*operands):
    dma = pltpu.SemaphoreType.DMA
    inside = pl.BlockSpec(memory_space=pltpu.VMEM)
    scalar = pl.BlockSpec(memory_space=pltpu.SMEM)
    shape = jax.ShapeDtypeStruct
    return pl.pallas_call(
        kernel,
        out_shape=(
            shape((128, 2048), BF16), shape((128, 2048), BF16), shape((64, 2, 384), F32),
            shape((64, 2, 384), F32), shape((2, 64, 128), F32), shape((2, 64, 128), F32),
        ),
        in_specs=[scalar] * 3 + [inside] * 10,
        out_specs=(inside,) * 6,
        scratch_shapes=[
            vm((2, 2, 128, 2048)), vm((2, 4, 4, 128, 128)),
            vm((8, 4, 128, 128)), vm((512, 1024)), vm((3, 2, 128, 256)), vm((8, 128, 256)),
            vm((2, 4, 4, 128, 128)), vm((8, 4, 128, 128)), vm((2, 128, 768)), vm((3, 2, 128, 256)),
            vm((3, 4, 2, 128, 256)), vm((3, 2, 128, 256)),
            vm((3, 3, 2, 128, 512)), vm((4, 128, 768), F32), vm((2, 128, 2048), F32),
            vm((3, 2, 128, 2048)), vm((3, 2, 2, 2, 16, 2048)), vm((3, 2, 2, 16, 2048)),
            vm((3, 2, 2, 16, 2048)), vm((3, 2, 2, 16, 2048)), vm((3, 2, 2, 16, 2048)),
            vm((3, 2, 128, 2048)), vm((2, 2, 16, 2048), F32), vm((2, 128, 256)),
            vm((3, 2, 128, 512), F32), vm((2, 2, 128, 512)), vm((2, 2, 128, 512)),
            vm((4, 4, 128, 256)), vm((4, 2, 128, 256)), vm((4, 2, 128, 256)), vm((4, 2, 2, 64, 256)),
            vm((8, 2048), F32), vm((2, 128, 768), F32),
            dma((8,)), dma((8,)), dma((3, 2, 2, 7)), dma((3, 2, 2, 7)),
            dma((8,)), dma((8,)), dma((8,)), dma((8,)), dma((8,)), dma((8,)),
            dma((3, 4)), dma((3, 4)), dma((4, 5)), dma((4, 2)), dma((4, 2, 2)),
        ],
        compiler_params=pltpu.CompilerParams(
            collective_id=0, has_side_effects=True, vmem_limit_bytes=VMEM_LIMIT
        ),
        name="step",
    )(*operands)


def finish_kernel(*refs):
    sources, targets, sems = refs[:6], refs[6:12], refs[12]
    leave = [pltpu.make_async_copy(x, y, sems.at[i]) for i, (x, y) in enumerate(zip(sources, targets))]
    for copy in leave:
        copy.start()
    for copy in leave:
        copy.wait()


def finish(*results):
    inside = pl.BlockSpec(memory_space=pltpu.VMEM)
    outside = pl.BlockSpec(memory_space=pl.ANY)
    return pl.pallas_call(
        finish_kernel,
        out_shape=tuple(jax.ShapeDtypeStruct(r.shape, r.dtype) for r in results),
        in_specs=[inside] * 6,
        out_specs=(outside,) * 6,
        scratch_shapes=[pltpu.SemaphoreType.DMA((6,))],
        compiler_params=pltpu.CompilerParams(vmem_limit_bytes=4 * 1024 * 1024),
        name="finish",
    )(*results)


def local(
    video_tokens, audio_tokens, qkv_video, out_video, qkv_audio, out_audio, gain_video, gain_audio,
    time_from, time_to, time_steps, windows, intersection,
):
    d_video, d_audio, qv, qa, ov, oa = finish(*fused(
        time_steps, windows, intersection.swapaxes(1, 2), video_tokens[0], audio_tokens[0],
        gain_video.reshape(1, 2048), gain_audio.reshape(1, 2048), time_from, time_to,
        qkv_video.reshape(2048, 768), qkv_audio.reshape(2048, 768),
        out_video.reshape(256, 2048), out_audio.reshape(256, 2048),
    ))
    return d_video[None], d_audio[None], qv, ov.swapaxes(1, 2), qa, oa.swapaxes(1, 2)


def solution(mesh):
    return jax.shard_map(
        local,
        mesh=mesh,
        in_specs=(
            P("clip", "vid", None), P("clip", "vid", None), P(None, "aud", None), P("aud", None, None),
            P(None, "aud", None), P("aud", None, None), P(), P(), P(), P(),
            P("clip", None), P("clip", None), P("clip", None, None),
        ),
        out_specs=(
            P("clip", "vid", None), P("clip", "vid", None), P(("clip", "vid"), "aud", None),
            P("aud", None, ("clip", "vid")), P(("clip", "vid"), "aud", None), P("aud", None, ("clip", "vid")),
        ),
        check_vma=False,
    )
```

```python
import jax
import jax.numpy as jnp
from jax import lax
from jax.experimental import pallas as pl
from jax.experimental.pallas import tpu as pltpu
from jax.sharding import PartitionSpec as P

BLK = 32
TGRID = 64
STEPS = 2
EPSILON = 1e-06
MESH = pl.DeviceIdType.MESH
F32 = jnp.float32
BF16 = jnp.bfloat16
NT = (((1,), (1,)), ((), ()))
TN = (((0,), (0,)), ((), ()))
NN = (((1,), (0,)), ((), ()))
T1, ST, T2 = 0, 1, 2
GG_EARLY = []
GG_LATE = [(0, 1), (1, 0), (3, 0), (1, 1), (3, 1), (2, 0), (2, 1)]
GROUPS = 2
PIECE = 32 // GROUPS
VMEM_LIMIT = 42 * 1024 * 1024


def dot(a, b, dims):
    return lax.dot_general(a, b, dims, preferred_element_type=F32)


def kernel(
    steps, windows, ranges, xv, xa, gv, ga, tf, tt, wqv, wqa, wov, woa,
    dv_out, da_out, qv_out, qa_out, ov_out, oa_out,
    N0, NS, NG, NGT, OB, OG, GS, GG, DQ, DG, QR, KV, PS, ACC,
    SB, R1, ZS, ZR, AG, DIFF, DO, DKV, DKS, DKR,
    WA, WR, WS, WF, WC, VR, VS, VF, MODS, BIAS,
    kv_s, kv_r, ar_s, ar_r, ng_s, ng_r, og_s, og_r, gg_s, gg_r,
    ed_s, ed_r, dg_s, dg_r, cl_s, cl_r, wf_r,
):
    v = lax.axis_index("vid")
    a = lax.axis_index("aud")
    c = lax.axis_index("clip")
    core = lax.rem(v, 2)
    yy = v // 2
    x = a // 2
    zh = lax.rem(a, 2)
    across = a + 1 - 2 * zh
    hops = (1, 3, 2)
    right = lax.rem(v + 1, 8)
    left = lax.rem(v + 7, 8)
    y_near = yy + 1 - 2 * lax.rem(yy, 2)
    y_far = 3 - yy
    y_one = (1 - core) * y_near + core * y_far
    y_two = core * y_near + (1 - core) * y_far
    y_last = 6 - yy - y_one - y_two
    mate = v + 1 - 2 * core

    def ahead(d):
        return lax.rem(x + d, 4)

    def piece(g, owner):
        return pl.ds(pl.multiple_of(PIECE * (4 * g + owner), PIECE), PIECE)

    chunks = [(g, m) for g in range(GROUPS) for m in range(2)]

    barrier = pltpu.get_barrier_semaphore()
    greet = [{"vid": lax.rem(v + d, 8)} for d in range(1, 8)]
    greet += [{"aud": peer} for peer in [2 * ahead(d) + zh for d in hops] + [across]]
    greet += [{"clip": c + 1 - 2 * lax.rem(c, 2)}]
    greet += [{"clip": lax.rem(c + 2, 4), "vid": 2 * yy + k} for k in range(2)]
    for peer in greet:
        pl.semaphore_signal(barrier, 1, device_id=peer, device_id_type=MESH)

    WQ = (wqv, wqa)
    WO = (wov, woa)
    pending = []

    def remote(src, dst, send, recv, device):
        return pltpu.make_async_remote_copy(
            src_ref=src, dst_ref=dst, send_sem=send, recv_sem=recv, device_id=device, device_id_type=MESH
        )

    def go(copy):
        copy.start()
        pending.append(copy)

    def wide(ref):
        return ref.astype(F32)

    now = steps[0, 0]
    stride = steps[0, 1]
    step = -stride.astype(F32) / TGRID
    conds = (
        tf[pl.ds(now, 1), :] + tt[pl.ds(now, 1), :],
        tf[pl.ds(now, 1), :] + tt[pl.ds(now - STEPS * stride, 1), :],
        tf[pl.ds(now - stride, 1), :] + tt[pl.ds(now - stride, 1), :],
    )
    gains = (gv, ga)
    for net in range(3):
        for m in range(2):
            MODS[2 * net + m : 2 * net + m + 1, :] = gains[m][...] * (1.0 + conds[net])

    xs = (xv, xa)

    def normed(net, m, r):
        part = pl.ds(pl.multiple_of(r * 32, 32), 32)
        cur = wide(xs[m][part, :])
        inv = lax.rsqrt(jnp.mean(cur * cur, -1, keepdims=True) + EPSILON)
        out = (cur * inv * MODS[2 * net + m : 2 * net + m + 1, :]).astype(BF16)
        N0[net, m, part, :] = out
        return part, out

    def make_qkv(net, rows_of, h):
        for m in range(2):
            rounded = dot(rows_of(m), WQ[m][:, 384 * h : 384 * h + 384], NN).astype(BF16)
            QR[net, m, :, 128 * h : 128 * h + 128] = rounded[:, 0:128]
            KV[net, h, 1, m] = rounded[:, 128:384]

    def kv_copies(net, h):
        return [
            remote(KV.at[net, h, 1], KV.at[net, h, 2 * k], kv_s.at[net, h, k], kv_r.at[net, h, k], {"vid": device})
            for k, device in enumerate((right, left))
        ]

    def kv_start(net, h):
        for copy in kv_copies(net, h):
            go(copy)

    def kv_wait(net, h):
        for copy in kv_copies(net, h):
            copy.wait_recv()

    for m in range(2):

        def norm_teacher(r, carry, m=m):
            normed(T1, m, r)
            return carry

        lax.fori_loop(0, 4, norm_teacher, 0)
    make_qkv(T1, lambda m: N0[T1, m], 0)
    pl.semaphore_wait(barrier, len(greet))
    kv_start(T1, 0)
    make_qkv(T1, lambda m: N0[T1, m], 1)
    kv_start(T1, 1)

    for m in range(2):

        def norm_student(r, carry, m=m):
            part, student = normed(ST, m, r)
            for s in range(16):
                NS[m, s // 4, s % 4, part, :] = student[:, 128 * s : 128 * s + 128]
            return carry

        lax.fori_loop(0, 4, norm_student, 0)
    for h in range(2):
        make_qkv(ST, lambda m: N0[ST, m], h)
        kv_start(ST, h)

    qpos = lax.broadcasted_iota(jnp.int32, (128, 128), 0)
    kpos = lax.broadcasted_iota(jnp.int32, (128, 128), 1)
    qblk = lax.broadcasted_iota(jnp.int32, (128, 1), 0) // BLK
    kblk = lax.broadcasted_iota(jnp.int32, (1, 128), 1) // BLK

    def spans(which, first_block, block_of):
        out = jnp.zeros(block_of.shape, jnp.int32)
        for i in range(4):
            at = jnp.clip(first_block + i, 0, 31)
            out = jnp.where(block_of == i, ranges[0, which, at], out)
        return out

    low_q = spans(0, 4 * v, qblk)
    high_q = spans(1, 4 * v, qblk)
    for slot in range(3):
        shard = v + slot - 1
        at = kpos + 128 * shard
        inside = (at >= 0) & (at < 1024)
        apart = jnp.abs(qpos - (kpos + 128 * (slot - 1)))
        keys_at = kblk + 4 * shard
        low_k = spans(0, 4 * shard, kblk)
        high_k = spans(1, 4 * shard, kblk)
        query_at = qblk + 4 * v
        tests = (
            (apart < windows[0, 0], (keys_at >= low_q) & (keys_at < high_q)),
            ((query_at >= low_k) & (query_at < high_k), apart < windows[0, 1]),
        )
        for m in range(2):
            for k in range(2):
                cols = slice(256 * slot + 128 * k, 256 * slot + 128 * k + 128)
                BIAS[m, :, cols] = jnp.where(inside & tests[m][k], 0.0, -1e30)

    def spread(src, dst, send, recv, offsets):
        for d in offsets:
            peer = 2 * lax.rem(yy + d[0], 4) + lax.rem(core + d[1], 2)
            go(remote(src(lax.rem(peer, 2), peer // 2), dst.at[v], send.at[peer], recv.at[v], {"vid": peer}))

    def collect(dst, send, recv):
        for d in range(1, 8):
            peer = lax.rem(v + d, 8)
            remote(dst.at[peer], dst.at[peer], send.at[peer], recv.at[peer], {"vid": peer}).wait_recv()

    whole = GG_EARLY + GG_LATE

    factor = 128 ** (-0.5)

    def attention(net, m, h, save=False):
        queries = QR[net, m, :, 128 * h : 128 * h + 128]
        keys = KV[net, h, :, :, :, 0:128].reshape(768, 128)
        values = KV[net, h, :, :, :, 128:256].reshape(768, 128)
        scores = dot(queries, keys, NT) * factor + BIAS[m]
        shifted = jnp.exp(scores - jnp.max(scores, -1, keepdims=True))
        prob = shifted * (1.0 / jnp.sum(shifted, -1, keepdims=True))
        if save:
            PS[2 * m + h] = prob
        OB[net, m, :, 128 * h : 128 * h + 128] = dot(prob.astype(BF16), values, NN).astype(BF16)

    def project_out(net, m):
        return dot(OB[net, m], WO[m][...], NN)

    def over_x(i, g, m, d, src, dst, kind):
        return remote(src, dst, ar_s.at[i, g, m, kind + d], ar_r.at[i, g, m, kind + d], {"aud": 2 * ahead(d) + zh})

    def over_z(i, g, m):
        return remote(ZS.at[i, g, m], ZR.at[i, g, m], ar_s.at[i, g, m, 0], ar_r.at[i, g, m, 0], {"aud": across})

    def sum_start(i, m):
        for g in range(GROUPS):
            for d in hops:
                go(over_x(i, g, m, d, SB.at[i, m, piece(g, ahead(d))], R1.at[i, g, m, d - 1], 0))

    def sum_on(i):
        for g, m in chunks:
            total = wide(SB[i, m, piece(g, x), :])
            for d in hops:
                over_x(i, g, m, d, R1.at[i, g, m, d - 1], R1.at[i, g, m, d - 1], 0).wait_recv()
                total = total + wide(R1[i, g, m, d - 1])
            ZS[i, g, m] = total.astype(BF16)
            go(over_z(i, g, m))

    def summed(i, g, m):
        over_z(i, g, m).wait_recv()
        return wide(ZS[i, g, m]) + wide(ZR[i, g, m])

    def share(i, g, m, value):
        AG[i, m, piece(g, x), :] = value.astype(BF16)
        part = AG.at[i, m, piece(g, x)]
        for d in hops:
            go(over_x(i, g, m, d, part, part, 3))

    def share_end(i):
        for g, m in chunks:
            for d in hops:
                part = AG.at[i, m, piece(g, ahead(4 - d))]
                over_x(i, g, m, d, part, part, 3).wait_recv()

    kv_wait(T1, 0)
    for m in range(2):
        attention(T1, m, 0)
    kv_wait(T1, 1)
    for m in range(2):
        attention(T1, m, 1)
        field = project_out(T1, m)
        SB[0, m] = field.astype(BF16)
        sum_start(0, m)
        ACC[m] = -field
    for h in range(2):
        kv_wait(ST, h)
    NG[v] = NS[core, :, yy]
    spread(lambda k, y: NS.at[k, :, y], NG, ng_s, ng_r, whole)
    for m in range(2):
        for h in range(2):
            attention(ST, m, h, True)
    OG[v] = OB[ST, core]
    spread(lambda k, y: OB.at[ST, k], OG, og_s, og_r, whole)
    sum_on(0)
    for m in range(2):
        ACC[m] = ACC[m] + 2.0 * project_out(ST, m)
    for g, m in chunks:
        cur = wide(xs[m][piece(g, x), :]) + step * summed(0, g, m)
        inv = lax.rsqrt(jnp.mean(cur * cur, -1, keepdims=True) + EPSILON)
        share(0, g, m, cur * inv * MODS[4 + m : 5 + m, :])
    share_end(0)

    for h in range(2):
        make_qkv(T2, lambda m: AG[0, m], h)
        kv_start(T2, h)
    kv_wait(T2, 0)
    for m in range(2):
        attention(T2, m, 0)
    kv_wait(T2, 1)
    for m in range(2):
        attention(T2, m, 1)
        SB[1, m] = (ACC[m] - project_out(T2, m)).astype(BF16)
        sum_start(1, m)
    collect(NG, ng_s, ng_r)
    for s in range(4):
        NGT[128 * s : 128 * s + 128, :] = NG[:, s].reshape(1024, 128).T
    collect(OG, og_s, og_r)
    sum_on(1)
    for g, m in chunks:
        diff = step * summed(1, g, m)
        DIFF[g, m] = diff
        share(1, g, m, 2.0 * step * diff)
    share_end(1)

    for m in range(2):
        DO[m] = dot(AG[1, m], WO[m][...], NT).astype(BF16)
    for m in range(2):
        for s in range(16):
            GS[m, s // 4, s % 4] = AG[1, m, :, 128 * s : 128 * s + 128]
    GG[v] = GS[core, :, yy]
    spread(lambda k, y: GS.at[k, :, y], GG, gg_s, gg_r, GG_EARLY)

    def backward(h):
        for m in range(2):
            queries = QR[ST, m, :, 128 * h : 128 * h + 128]
            keys = KV[ST, h, :, :, :, 0:128].reshape(768, 128)
            values = KV[ST, h, :, :, :, 128:256].reshape(768, 128)
            grad_out = DO[m, :, 128 * h : 128 * h + 128]
            prob = PS[2 * m + h]
            grad_prob = dot(grad_out, values, NT)
            center = jnp.sum(prob * grad_prob, -1, keepdims=True)
            dscore = (prob * (grad_prob - center) * factor).astype(BF16)
            DQ[h, m, :, 0:128] = dot(dscore, keys, NN).astype(BF16)
            dkey = dot(dscore, queries, TN).reshape(3, 2, 128, 128)
            dvalue = dot(prob.astype(BF16), grad_out, TN).reshape(3, 2, 128, 128)
            if m == 0:
                DKV[h, :, :, :, 0:128] = dkey
                DKV[h, :, :, :, 128:256] = dvalue
            else:
                for slot in (0, 2):
                    DKS[h, slot // 2, :, :, 0:128] = (DKV[h, slot, :, :, 0:128] + dkey[slot]).astype(BF16)
                    DKS[h, slot // 2, :, :, 128:256] = (DKV[h, slot, :, :, 128:256] + dvalue[slot]).astype(BF16)
                DKV[h, 1, :, :, 0:128] = DKV[h, 1, :, :, 0:128] + dkey[1]
                DKV[h, 1, :, :, 128:256] = DKV[h, 1, :, :, 128:256] + dvalue[1]

    def edges(h):
        return [
            remote(DKS.at[h, k], DKR.at[h, k], ed_s.at[h, k], ed_r.at[h, k], {"vid": device})
            for k, device in enumerate((left, right))
        ]

    def finish_kv(h):
        for copy in edges(h):
            copy.wait_recv()
        for m in range(2):
            DQ[h, m, :, 128:384] = (DKV[h, 1, m] + wide(DKR[h, 0, m]) + wide(DKR[h, 1, m])).astype(BF16)

    def line(n, k, part, device):
        return remote(part, part, dg_s.at[n, k], dg_r.at[n, k], {"vid": device})

    def line_start(n):
        DG[n, yy, core] = DQ[n, core]
        go(remote(DQ.at[n, 1 - core], DG.at[n, yy, core], dg_s.at[n, 0], dg_r.at[n, 0], {"vid": mate}))

    def line_send(n):
        line(n, 0, DG.at[n, yy, 1 - core], mate).wait_recv()
        go(line(n, 1, DG.at[n, yy], 2 * y_one + core))
        go(line(n, 2, DG.at[n, yy], 2 * y_two + core))

    def line_on(n):
        line(n, 1, DG.at[n, y_one], 2 * y_one + core).wait_recv()
        go(line(n, 3, DG.at[n, y_one], 2 * y_two + core))

    def line_end(n):
        line(n, 2, DG.at[n, y_two], 2 * y_two + core).wait_recv()
        line(n, 3, DG.at[n, y_last], 2 * y_two + core).wait_recv()

    for h in range(2):
        backward(h)
        for copy in edges(h):
            go(copy)
    finish_kv(0)
    line_start(0)
    for m in range(2):
        ACC[m] = dot(DQ[0, m], WQ[m][:, 0:384], NT)
    line_send(0)
    finish_kv(1)
    line_start(1)
    for m in range(2):
        SB[2, m] = (ACC[m] + dot(DQ[1, m], WQ[m][:, 384:768], NT)).astype(BF16)
        sum_start(2, m)
        if m == 0:
            line_send(1)
    line_on(0)

    c_one = c + 1 - 2 * lax.rem(c, 2)
    c_two = lax.rem(c + 2, 4)
    c_not = lax.rem(c_one + 2, 4)
    mine = pl.ds(pl.multiple_of(64 * core, 64), 64)
    theirs = pl.ds(pl.multiple_of(64 * (1 - core), 64), 64)

    parts = ((WA.at[0], WR.at[0], WS.at[0], WF.at[0]), (WA.at[1], WR.at[1], WS.at[1], WF.at[1]), (WC, VR, VS, VF))

    def clip_start(n):
        full, got, out, last = parts[n]
        for k, block in ((1, c_not), (0, c_one)):
            go(remote(full.at[block], got.at[k], cl_s.at[n, k], cl_r.at[n, k], {"clip": c_one}))

    def clip_on(n):
        full, got, out, last = parts[n]
        for k, block in ((1, c_two), (0, c)):
            part = got.at[k]
            remote(part, part, cl_s.at[n, k], cl_r.at[n, k], {"clip": c_one}).wait_recv()
            out[k] = (wide(full[block]) + wide(got[k])).astype(BF16)
            if k == 1:
                for j, half, device in ((2, mine, {"clip": c_two}), (3, theirs, {"clip": c_two, "vid": mate})):
                    go(remote(out.at[1, half], last.at[core, 1], cl_s.at[n, j], wf_r.at[n, core, 1], device))
            else:
                go(remote(out.at[0, theirs], last.at[core, 0], cl_s.at[n, 4], wf_r.at[n, core, 0], {"vid": mate}))
                last[core, 0] = out[0, mine, :]

    def clip_end(n):
        last = parts[n][3]
        for src, k, device in (
            (core, 1, {"clip": c_two}), (1 - core, 1, {"clip": c_two, "vid": mate}), (1 - core, 0, {"vid": mate})
        ):
            part = last.at[src, k]
            remote(part, part, cl_s.at[n, 2], wf_r.at[n, src, k], device).wait_recv()
        return [wide(last[m, 0]) + wide(last[m, 1]) for m in range(2)]

    def line_grad(n):
        line_end(n)
        WA[n] = dot(NGT[...], DG[n].reshape(1024, 384), NN).astype(BF16).reshape(4, 128, 384)
        clip_start(n)

    line_on(1)
    spread(lambda k, y: GS.at[k, :, y], GG, gg_s, gg_r, GG_LATE)
    sum_on(2)
    line_grad(0)
    line_grad(1)
    clip_on(0)
    for g, m in chunks:
        cur = wide(xs[m][piece(g, x), :])
        inv = lax.rsqrt(jnp.mean(cur * cur, -1, keepdims=True) + EPSILON)
        scaled = summed(2, g, m) * MODS[2 + m : 3 + m, :]
        back = inv * scaled - cur * (inv * inv * inv) * jnp.mean(scaled * cur, -1, keepdims=True)
        share(2, g, m, DIFF[g, m] + back)
    collect(GG, gg_s, gg_r)
    o_all = OG[...].reshape(1024, 256)
    for s in range(4):
        WC[s] = dot(GG[:, s].reshape(1024, 128), o_all, TN).astype(BF16)
    clip_start(2)
    clip_on(1)
    clip_on(2)
    q_outs = (qv_out, qa_out)
    o_outs = (ov_out, oa_out)
    for h in range(2):
        for m, total in enumerate(clip_end(h)):
            q_outs[m][:, h, :] = total
    share_end(2)
    dv_out[...] = AG[2, 0]
    da_out[...] = AG[2, 1]
    for m, total in enumerate(clip_end(2)):
        for h in range(2):
            o_outs[m][h] = total[:, 128 * h : 128 * h + 128]
    for copy in pending:
        copy.wait_send()


def vm(shape, kind=BF16):
    return pltpu.VMEM(shape, kind)


def fused(*operands):
    dma = pltpu.SemaphoreType.DMA
    inside = pl.BlockSpec(memory_space=pltpu.VMEM)
    scalar = pl.BlockSpec(memory_space=pltpu.SMEM)
    shape = jax.ShapeDtypeStruct
    return pl.pallas_call(
        kernel,
        out_shape=(
            shape((128, 2048), BF16), shape((128, 2048), BF16), shape((64, 2, 384), F32),
            shape((64, 2, 384), F32), shape((2, 64, 128), F32), shape((2, 64, 128), F32),
        ),
        in_specs=[scalar] * 3 + [inside] * 10,
        out_specs=(inside,) * 6,
        scratch_shapes=[
            vm((2, 2, 128, 2048)), vm((2, 4, 4, 128, 128)),
            vm((8, 4, 128, 128)), vm((512, 1024)), vm((3, 2, 128, 256)), vm((8, 128, 256)),
            vm((2, 4, 4, 128, 128)), vm((8, 4, 128, 128)), vm((2, 2, 128, 384)),
            vm((2, 4, 2, 128, 384)), vm((3, 2, 128, 256)),
            vm((3, 2, 3, 2, 128, 256)), vm((4, 128, 768), F32), vm((2, 128, 2048), F32),
            vm((3, 2, 128, 2048)), vm((3, GROUPS, 2, 3, PIECE, 2048)),
            vm((3, GROUPS, 2, PIECE, 2048)), vm((3, GROUPS, 2, PIECE, 2048)),
            vm((3, 2, 128, 2048)), vm((GROUPS, 2, PIECE, 2048), F32), vm((2, 128, 256)),
            vm((2, 3, 2, 128, 256), F32), vm((2, 2, 2, 128, 256)), vm((2, 2, 2, 128, 256)),
            vm((2, 4, 128, 384)), vm((2, 2, 128, 384)), vm((2, 2, 128, 384)), vm((2, 2, 2, 64, 384)),
            vm((4, 128, 256)), vm((2, 128, 256)), vm((2, 128, 256)), vm((2, 2, 64, 256)),
            vm((8, 2048), F32), vm((2, 128, 768), F32),
            dma((3, 2, 2)), dma((3, 2, 2)), dma((3, GROUPS, 2, 7)), dma((3, GROUPS, 2, 7)),
            dma((8,)), dma((8,)), dma((8,)), dma((8,)), dma((8,)), dma((8,)),
            dma((2, 2)), dma((2, 2)), dma((2, 4)), dma((2, 4)), dma((3, 5)), dma((3, 2)), dma((3, 2, 2)),
        ],
        compiler_params=pltpu.CompilerParams(
            collective_id=0, has_side_effects=True, vmem_limit_bytes=VMEM_LIMIT
        ),
        name="step",
    )(*operands)


def finish_kernel(*refs):
    sources, targets, sems = refs[:6], refs[6:12], refs[12]
    leave = [pltpu.make_async_copy(x, y, sems.at[i]) for i, (x, y) in enumerate(zip(sources, targets))]
    for copy in leave:
        copy.start()
    for copy in leave:
        copy.wait()


def finish(*results):
    inside = pl.BlockSpec(memory_space=pltpu.VMEM)
    outside = pl.BlockSpec(memory_space=pl.ANY)
    return pl.pallas_call(
        finish_kernel,
        out_shape=tuple(jax.ShapeDtypeStruct(r.shape, r.dtype) for r in results),
        in_specs=[inside] * 6,
        out_specs=(outside,) * 6,
        scratch_shapes=[pltpu.SemaphoreType.DMA((6,))],
        compiler_params=pltpu.CompilerParams(vmem_limit_bytes=4 * 1024 * 1024),
        name="finish",
    )(*results)


def local(
    video_tokens, audio_tokens, qkv_video, out_video, qkv_audio, out_audio, gain_video, gain_audio,
    time_from, time_to, time_steps, windows, intersection,
):
    d_video, d_audio, qv, qa, ov, oa = finish(*fused(
        time_steps, windows, intersection.swapaxes(1, 2), video_tokens[0], audio_tokens[0],
        gain_video.reshape(1, 2048), gain_audio.reshape(1, 2048), time_from, time_to,
        qkv_video.reshape(2048, 768), qkv_audio.reshape(2048, 768),
        out_video.reshape(256, 2048), out_audio.reshape(256, 2048),
    ))
    return d_video[None], d_audio[None], qv, ov.swapaxes(1, 2), qa, oa.swapaxes(1, 2)


def solution(mesh):
    return jax.shard_map(
        local,
        mesh=mesh,
        in_specs=(
            P("clip", "vid", None), P("clip", "vid", None), P(None, "aud", None), P("aud", None, None),
            P(None, "aud", None), P("aud", None, None), P(), P(), P(), P(),
            P("clip", None), P("clip", None), P("clip", None, None),
        ),
        out_specs=(
            P("clip", "vid", None), P("clip", "vid", None), P(("clip", "vid"), "aud", None),
            P("aud", None, ("clip", "vid")), P(("clip", "vid"), "aud", None), P("aud", None, ("clip", "vid")),
        ),
        check_vma=False,
    )
```

```python
import jax
import jax.numpy as jnp
from jax import lax
from jax.experimental import pallas as pl
from jax.experimental.pallas import tpu as pltpu
from jax.sharding import PartitionSpec as P

BLK = 32
TGRID = 64
STEPS = 2
EPSILON = 1e-06
MESH = pl.DeviceIdType.MESH
F32 = jnp.float32
BF16 = jnp.bfloat16
NT = (((1,), (1,)), ((), ()))
TN = (((0,), (0,)), ((), ()))
NN = (((1,), (0,)), ((), ()))
T1, ST, T2 = 0, 1, 2
GROUPS = 2
PIECE = 32 // GROUPS
VMEM_LIMIT = 42 * 1024 * 1024


def dot(a, b, dims):
    return lax.dot_general(a, b, dims, preferred_element_type=F32)


def kernel(
    steps, windows, ranges, xv, xa, gv, ga, tf, tt, wqv, wqa, wov, woa,
    dv_out, da_out, qv_out, qa_out, ov_out, oa_out,
    N0, NS, NG, NGT, OB, OG, GS, GG, DQ, DG, QR, KV, PS, PT, ACC,
    SB, R1, ZS, ZR, AG, DIFF, DO, DKV, DKS, DKR,
    WA, WR, WS, WF, WC, VR, VS, VF, MODS, BIAS,
    kv_s, kv_r, ar_s, ar_r, ng_s, ng_r, og_s, og_r, gg_s, gg_r,
    ed_s, ed_r, dg_s, dg_r, cl_s, cl_r, wf_r,
):
    v = lax.axis_index("vid")
    a = lax.axis_index("aud")
    c = lax.axis_index("clip")
    core = lax.rem(v, 2)
    yy = v // 2
    x = a // 2
    zh = lax.rem(a, 2)
    across = a + 1 - 2 * zh
    hops = (1, 3, 2)
    right = lax.rem(v + 1, 8)
    left = lax.rem(v + 7, 8)
    y_near = yy + 1 - 2 * lax.rem(yy, 2)
    y_far = 3 - yy
    y_one = (1 - core) * y_near + core * y_far
    y_two = core * y_near + (1 - core) * y_far
    y_last = 6 - yy - y_one - y_two
    mate = v + 1 - 2 * core

    def ahead(d):
        return lax.rem(x + d, 4)

    def piece(g, owner):
        return pl.ds(pl.multiple_of(PIECE * (4 * g + owner), PIECE), PIECE)

    chunks = [(g, m) for m in range(2) for g in range(GROUPS)]

    barrier = pltpu.get_barrier_semaphore()
    greet = [{"vid": lax.rem(v + d, 8)} for d in range(1, 8)]
    greet += [{"aud": peer} for peer in [2 * ahead(d) + zh for d in hops] + [across]]
    greet += [{"clip": c + 1 - 2 * lax.rem(c, 2)}]
    greet += [{"clip": lax.rem(c + 2, 4), "vid": 2 * yy + k} for k in range(2)]
    for peer in greet:
        pl.semaphore_signal(barrier, 1, device_id=peer, device_id_type=MESH)

    WQ = (wqv, wqa)
    WO = (wov, woa)
    pending = []

    def remote(src, dst, send, recv, device):
        return pltpu.make_async_remote_copy(
            src_ref=src, dst_ref=dst, send_sem=send, recv_sem=recv, device_id=device, device_id_type=MESH
        )

    def go(copy):
        copy.start()
        pending.append(copy)

    def wide(ref):
        return ref.astype(F32)

    now = steps[0, 0]
    stride = steps[0, 1]
    step = -stride.astype(F32) / TGRID
    conds = (
        tf[pl.ds(now, 1), :] + tt[pl.ds(now, 1), :],
        tf[pl.ds(now, 1), :] + tt[pl.ds(now - STEPS * stride, 1), :],
        tf[pl.ds(now - stride, 1), :] + tt[pl.ds(now - stride, 1), :],
    )
    gains = (gv, ga)
    for net in range(3):
        for m in range(2):
            MODS[2 * net + m : 2 * net + m + 1, :] = gains[m][...] * (1.0 + conds[net])

    xs = (xv, xa)

    def normed(net, m, r):
        part = pl.ds(pl.multiple_of(r * 32, 32), 32)
        cur = wide(xs[m][part, :])
        inv = lax.rsqrt(jnp.mean(cur * cur, -1, keepdims=True) + EPSILON)
        out = (cur * inv * MODS[2 * net + m : 2 * net + m + 1, :]).astype(BF16)
        N0[net, m, part, :] = out
        return part, out

    def make_qkv(net, rows, h, m):
        rounded = dot(rows, WQ[m][:, 384 * h : 384 * h + 384], NN).astype(BF16)
        QR[net, m, :, 128 * h : 128 * h + 128] = rounded[:, 0:128]
        KV[net, h, 1, m] = rounded[:, 128:384]

    def kv_copies(net, h, m):
        sent = KV.at[net, h, 1, m]
        return [
            remote(sent, KV.at[net, h, 2 * k, m], kv_s.at[net, h, m, k], kv_r.at[net, h, m, k], {"vid": device})
            for k, device in enumerate((right, left))
        ]

    def kv_start(net, h, m):
        for copy in kv_copies(net, h, m):
            go(copy)

    def kv_wait(net, h):
        for m in range(2):
            for copy in kv_copies(net, h, m):
                copy.wait_recv()

    for m in range(2):

        def norm_teacher(r, carry, m=m):
            normed(T1, m, r)
            return carry

        lax.fori_loop(0, 4, norm_teacher, 0)
    for m in range(2):
        make_qkv(T1, N0[T1, m], 0, m)
    pl.semaphore_wait(barrier, len(greet))
    for m in range(2):
        kv_start(T1, 0, m)
    for m in range(2):
        make_qkv(T1, N0[T1, m], 1, m)
        kv_start(T1, 1, m)

    for m in range(2):

        def norm_student(r, carry, m=m):
            part, student = normed(ST, m, r)
            for s in range(16):
                NS[m, s // 4, s % 4, part, :] = student[:, 128 * s : 128 * s + 128]
            return carry

        lax.fori_loop(0, 4, norm_student, 0)
    for h in range(2):
        for m in range(2):
            make_qkv(ST, N0[ST, m], h, m)
            kv_start(ST, h, m)

    qpos = lax.broadcasted_iota(jnp.int32, (128, 128), 0)
    kpos = lax.broadcasted_iota(jnp.int32, (128, 128), 1)
    qblk = lax.broadcasted_iota(jnp.int32, (128, 1), 0) // BLK
    kblk = lax.broadcasted_iota(jnp.int32, (1, 128), 1) // BLK

    def spans(which, first_block, block_of):
        out = jnp.zeros(block_of.shape, jnp.int32)
        for i in range(4):
            at = jnp.clip(first_block + i, 0, 31)
            out = jnp.where(block_of == i, ranges[0, which, at], out)
        return out

    low_q = spans(0, 4 * v, qblk)
    high_q = spans(1, 4 * v, qblk)
    for slot in range(3):
        shard = v + slot - 1
        at = kpos + 128 * shard
        inside = (at >= 0) & (at < 1024)
        apart = jnp.abs(qpos - (kpos + 128 * (slot - 1)))
        keys_at = kblk + 4 * shard
        low_k = spans(0, 4 * shard, kblk)
        high_k = spans(1, 4 * shard, kblk)
        query_at = qblk + 4 * v
        tests = (
            (apart < windows[0, 0], (keys_at >= low_q) & (keys_at < high_q)),
            ((query_at >= low_k) & (query_at < high_k), apart < windows[0, 1]),
        )
        for m in range(2):
            for k in range(2):
                cols = slice(256 * slot + 128 * k, 256 * slot + 128 * k + 128)
                BIAS[m, :, cols] = jnp.where(inside & tests[m][k], 0.0, -1e30)

    def spread(src, dst, send, recv, offsets):
        for d in offsets:
            peer = 2 * lax.rem(yy + d[0], 4) + lax.rem(core + d[1], 2)
            go(remote(src(lax.rem(peer, 2), peer // 2), dst.at[v], send.at[peer], recv.at[v], {"vid": peer}))

    def collect(dst, send, recv):
        for d in range(1, 8):
            peer = lax.rem(v + d, 8)
            remote(dst.at[peer], dst.at[peer], send.at[peer], recv.at[peer], {"vid": peer}).wait_recv()

    whole = [(0, 1), (1, 0), (3, 0), (1, 1), (3, 1), (2, 0), (2, 1)]

    factor = 128 ** (-0.5)

    def attention(net, m, h, save=False):
        queries = QR[net, m, :, 128 * h : 128 * h + 128]
        keys = KV[net, h, :, :, :, 0:128].reshape(768, 128)
        values = KV[net, h, :, :, :, 128:256].reshape(768, 128)
        scores = dot(queries, keys, NT) * factor + BIAS[m]
        shifted = jnp.exp(scores - jnp.max(scores, -1, keepdims=True))
        prob = shifted * (1.0 / jnp.sum(shifted, -1, keepdims=True))
        if save:
            PS[2 * m + h] = prob
        OB[net, m, :, 128 * h : 128 * h + 128] = dot(prob.astype(BF16), values, NN).astype(BF16)

    def project_out(net, m):
        return dot(OB[net, m], WO[m][...], NN)

    def over_x(i, g, m, d, src, dst, kind):
        return remote(src, dst, ar_s.at[i, g, m, kind + d], ar_r.at[i, g, m, kind + d], {"aud": 2 * ahead(d) + zh})

    def over_z(i, g, m):
        return remote(ZS.at[i, g, m], ZR.at[i, g, m], ar_s.at[i, g, m, 0], ar_r.at[i, g, m, 0], {"aud": across})

    def sum_start(i, m):
        for g in range(GROUPS):
            for d in hops:
                go(over_x(i, g, m, d, SB.at[i, m, piece(g, ahead(d))], R1.at[i, g, m, d - 1], 0))

    def sum_on(i):
        for g, m in chunks:
            total = wide(SB[i, m, piece(g, x), :])
            for d in hops:
                over_x(i, g, m, d, R1.at[i, g, m, d - 1], R1.at[i, g, m, d - 1], 0).wait_recv()
                total = total + wide(R1[i, g, m, d - 1])
            ZS[i, g, m] = total.astype(BF16)
            go(over_z(i, g, m))

    def summed(i, g, m):
        over_z(i, g, m).wait_recv()
        return wide(ZS[i, g, m]) + wide(ZR[i, g, m])

    def share(i, g, m, value):
        AG[i, m, piece(g, x), :] = value.astype(BF16)
        part = AG.at[i, m, piece(g, x)]
        for d in hops:
            go(over_x(i, g, m, d, part, part, 3))

    def share_end(i, m):
        for g in range(GROUPS):
            for d in hops:
                part = AG.at[i, m, piece(g, ahead(4 - d))]
                over_x(i, g, m, d, part, part, 3).wait_recv()

    kv_wait(T1, 0)
    for m in range(2):
        attention(T1, m, 0)
    kv_wait(T1, 1)
    for m in range(2):
        attention(T1, m, 1)
        field = project_out(T1, m)
        SB[0, m] = field.astype(BF16)
        sum_start(0, m)
        ACC[m] = -field
    for h in range(2):
        kv_wait(ST, h)
    NG[v] = NS[core, :, yy]
    spread(lambda k, y: NS.at[k, :, y], NG, ng_s, ng_r, whole)
    for m in range(2):
        for h in range(2):
            attention(ST, m, h, True)
    OG[v] = OB[ST, core]
    spread(lambda k, y: OB.at[ST, k], OG, og_s, og_r, whole)
    sum_on(0)
    for m in range(2):
        ACC[m] = ACC[m] + 2.0 * project_out(ST, m)
    for g, m in chunks:
        cur = wide(xs[m][piece(g, x), :]) + step * summed(0, g, m)
        inv = lax.rsqrt(jnp.mean(cur * cur, -1, keepdims=True) + EPSILON)
        share(0, g, m, cur * inv * MODS[4 + m : 5 + m, :])

    for m in range(2):
        share_end(0, m)
        for h in range(2):
            make_qkv(T2, AG[0, m], h, m)
            kv_start(T2, h, m)
    kv_wait(T2, 0)
    for m in range(2):
        attention(T2, m, 0)
    kv_wait(T2, 1)
    for m in range(2):
        attention(T2, m, 1)
        SB[1, m] = (ACC[m] - project_out(T2, m)).astype(BF16)
        sum_start(1, m)
    for m in range(2):
        for h in range(2):
            PT[2 * m + h] = PS[2 * m + h].astype(BF16).T
    collect(NG, ng_s, ng_r)
    for s in range(4):
        NGT[128 * s : 128 * s + 128, :] = NG[:, s].reshape(1024, 128).T
    collect(OG, og_s, og_r)
    sum_on(1)
    for g, m in chunks:
        diff = step * summed(1, g, m)
        DIFF[g, m] = diff
        share(1, g, m, 2.0 * step * diff)

    def backward(h, m):
        queries = QR[ST, m, :, 128 * h : 128 * h + 128]
        keys = KV[ST, h, :, :, :, 0:128].reshape(768, 128)
        values = KV[ST, h, :, :, :, 128:256].reshape(768, 128)
        grad_out = DO[m, :, 128 * h : 128 * h + 128]
        prob = PS[2 * m + h]
        grad_prob = dot(grad_out, values, NT)
        center = jnp.sum(prob * grad_prob, -1, keepdims=True)
        dscore = (prob * (grad_prob - center) * factor).astype(BF16)
        DQ[h, m, :, 0:128] = dot(dscore, keys, NN).astype(BF16)
        dkey = dot(dscore, queries, TN).reshape(3, 2, 128, 128)
        dvalue = dot(PT[2 * m + h], grad_out, NN).reshape(3, 2, 128, 128)
        if m == 0:
            DKV[h, :, :, :, 0:128] = dkey
            DKV[h, :, :, :, 128:256] = dvalue
        else:
            for slot in (0, 2):
                DKS[h, slot // 2, :, :, 0:128] = (DKV[h, slot, :, :, 0:128] + dkey[slot]).astype(BF16)
                DKS[h, slot // 2, :, :, 128:256] = (DKV[h, slot, :, :, 128:256] + dvalue[slot]).astype(BF16)
            DKV[h, 1, :, :, 0:128] = DKV[h, 1, :, :, 0:128] + dkey[1]
            DKV[h, 1, :, :, 128:256] = DKV[h, 1, :, :, 128:256] + dvalue[1]

    def edges(h):
        return [
            remote(DKS.at[h, k], DKR.at[h, k], ed_s.at[h, k], ed_r.at[h, k], {"vid": device})
            for k, device in enumerate((left, right))
        ]

    def finish_kv(h):
        for copy in edges(h):
            copy.wait_recv()
        for m in range(2):
            DQ[h, m, :, 128:384] = (DKV[h, 1, m] + wide(DKR[h, 0, m]) + wide(DKR[h, 1, m])).astype(BF16)

    def line(n, k, part, device):
        return remote(part, part, dg_s.at[n, k], dg_r.at[n, k], {"vid": device})

    def line_start(n):
        DG[n, yy, core] = DQ[n, core]
        go(remote(DQ.at[n, 1 - core], DG.at[n, yy, core], dg_s.at[n, 0], dg_r.at[n, 0], {"vid": mate}))

    def line_send(n):
        line(n, 0, DG.at[n, yy, 1 - core], mate).wait_recv()
        go(line(n, 1, DG.at[n, yy], 2 * y_one + core))
        go(line(n, 2, DG.at[n, yy], 2 * y_two + core))

    def line_on(n):
        line(n, 1, DG.at[n, y_one], 2 * y_one + core).wait_recv()
        go(line(n, 3, DG.at[n, y_one], 2 * y_two + core))

    def line_end(n):
        line(n, 2, DG.at[n, y_two], 2 * y_two + core).wait_recv()
        line(n, 3, DG.at[n, y_last], 2 * y_two + core).wait_recv()

    for m in range(2):
        share_end(1, m)
        DO[m] = dot(AG[1, m], WO[m][...], NT).astype(BF16)
        for h in range(2):
            backward(h, m)
            if m == 1:
                for copy in edges(h):
                    go(copy)
    finish_kv(0)
    line_start(0)
    for m in range(2):
        ACC[m] = dot(DQ[0, m], WQ[m][:, 0:384], NT)
    line_send(0)
    finish_kv(1)
    line_start(1)
    for m in range(2):
        SB[2, m] = (ACC[m] + dot(DQ[1, m], WQ[m][:, 384:768], NT)).astype(BF16)
        sum_start(2, m)
        if m == 0:
            line_send(1)
    line_on(0)

    c_one = c + 1 - 2 * lax.rem(c, 2)
    c_two = lax.rem(c + 2, 4)
    c_not = lax.rem(c_one + 2, 4)
    mine = pl.ds(pl.multiple_of(64 * core, 64), 64)
    theirs = pl.ds(pl.multiple_of(64 * (1 - core), 64), 64)

    parts = ((WA.at[0], WR.at[0], WS.at[0], WF.at[0]), (WA.at[1], WR.at[1], WS.at[1], WF.at[1]), (WC, VR, VS, VF))

    def clip_start(n):
        full, got, out, last = parts[n]
        for k, block in ((1, c_not), (0, c_one)):
            go(remote(full.at[block], got.at[k], cl_s.at[n, k], cl_r.at[n, k], {"clip": c_one}))

    def clip_on(n):
        full, got, out, last = parts[n]
        for k, block in ((1, c_two), (0, c)):
            part = got.at[k]
            remote(part, part, cl_s.at[n, k], cl_r.at[n, k], {"clip": c_one}).wait_recv()
            out[k] = (wide(full[block]) + wide(got[k])).astype(BF16)
            if k == 1:
                for j, half, device in ((2, mine, {"clip": c_two}), (3, theirs, {"clip": c_two, "vid": mate})):
                    go(remote(out.at[1, half], last.at[core, 1], cl_s.at[n, j], wf_r.at[n, core, 1], device))
            else:
                go(remote(out.at[0, theirs], last.at[core, 0], cl_s.at[n, 4], wf_r.at[n, core, 0], {"vid": mate}))
                last[core, 0] = out[0, mine, :]

    def clip_end(n):
        last = parts[n][3]
        for src, k, device in (
            (core, 1, {"clip": c_two}), (1 - core, 1, {"clip": c_two, "vid": mate}), (1 - core, 0, {"vid": mate})
        ):
            part = last.at[src, k]
            remote(part, part, cl_s.at[n, 2], wf_r.at[n, src, k], device).wait_recv()
        return [wide(last[m, 0]) + wide(last[m, 1]) for m in range(2)]

    def line_grad(n):
        line_end(n)
        WA[n] = dot(NGT[...], DG[n].reshape(1024, 384), NN).astype(BF16).reshape(4, 128, 384)
        clip_start(n)

    line_on(1)
    for m in range(2):
        for s in range(16):
            GS[m, s // 4, s % 4] = AG[1, m, :, 128 * s : 128 * s + 128]
    GG[v] = GS[core, :, yy]
    spread(lambda k, y: GS.at[k, :, y], GG, gg_s, gg_r, whole)
    sum_on(2)
    line_grad(0)
    def back_on(m):
        for g in range(GROUPS):
            cur = wide(xs[m][piece(g, x), :])
            inv = lax.rsqrt(jnp.mean(cur * cur, -1, keepdims=True) + EPSILON)
            scaled = summed(2, g, m) * MODS[2 + m : 3 + m, :]
            back = inv * scaled - cur * (inv * inv * inv) * jnp.mean(scaled * cur, -1, keepdims=True)
            share(2, g, m, DIFF[g, m] + back)

    back_on(0)
    line_grad(1)
    clip_on(0)
    back_on(1)
    collect(GG, gg_s, gg_r)
    o_all = OG[...].reshape(1024, 256)
    for s in range(4):
        WC[s] = dot(GG[:, s].reshape(1024, 128), o_all, TN).astype(BF16)
    clip_start(2)
    clip_on(1)
    clip_on(2)
    q_outs = (qv_out, qa_out)
    o_outs = (ov_out, oa_out)
    for h in range(2):
        for m, total in enumerate(clip_end(h)):
            q_outs[m][:, h, :] = total
    for m in range(2):
        share_end(2, m)
    dv_out[...] = AG[2, 0]
    da_out[...] = AG[2, 1]
    for m, total in enumerate(clip_end(2)):
        for h in range(2):
            o_outs[m][h] = total[:, 128 * h : 128 * h + 128]
    for copy in pending:
        copy.wait_send()


def vm(shape, kind=BF16):
    return pltpu.VMEM(shape, kind)


def fused(*operands):
    dma = pltpu.SemaphoreType.DMA
    inside = pl.BlockSpec(memory_space=pltpu.VMEM)
    scalar = pl.BlockSpec(memory_space=pltpu.SMEM)
    shape = jax.ShapeDtypeStruct
    return pl.pallas_call(
        kernel,
        out_shape=(
            shape((128, 2048), BF16), shape((128, 2048), BF16), shape((64, 2, 384), F32),
            shape((64, 2, 384), F32), shape((2, 64, 128), F32), shape((2, 64, 128), F32),
        ),
        in_specs=[scalar] * 3 + [inside] * 10,
        out_specs=(inside,) * 6,
        scratch_shapes=[
            vm((2, 2, 128, 2048)), vm((2, 4, 4, 128, 128)),
            vm((8, 4, 128, 128)), vm((512, 1024)), vm((3, 2, 128, 256)), vm((8, 128, 256)),
            vm((2, 4, 4, 128, 128)), vm((8, 4, 128, 128)), vm((2, 2, 128, 384)),
            vm((2, 4, 2, 128, 384)), vm((3, 2, 128, 256)),
            vm((3, 2, 3, 2, 128, 256)), vm((4, 128, 768), F32), vm((4, 768, 128)), vm((2, 128, 2048), F32),
            vm((3, 2, 128, 2048)), vm((3, GROUPS, 2, 3, PIECE, 2048)),
            vm((3, GROUPS, 2, PIECE, 2048)), vm((3, GROUPS, 2, PIECE, 2048)),
            vm((3, 2, 128, 2048)), vm((GROUPS, 2, PIECE, 2048), F32), vm((2, 128, 256)),
            vm((2, 3, 2, 128, 256), F32), vm((2, 2, 2, 128, 256)), vm((2, 2, 2, 128, 256)),
            vm((2, 4, 128, 384)), vm((2, 2, 128, 384)), vm((2, 2, 128, 384)), vm((2, 2, 2, 64, 384)),
            vm((4, 128, 256)), vm((2, 128, 256)), vm((2, 128, 256)), vm((2, 2, 64, 256)),
            vm((8, 2048), F32), vm((2, 128, 768), F32),
            dma((3, 2, 2, 2)), dma((3, 2, 2, 2)), dma((3, GROUPS, 2, 7)), dma((3, GROUPS, 2, 7)),
            dma((8,)), dma((8,)), dma((8,)), dma((8,)), dma((8,)), dma((8,)),
            dma((2, 2)), dma((2, 2)), dma((2, 4)), dma((2, 4)), dma((3, 5)), dma((3, 2)), dma((3, 2, 2)),
        ],
        compiler_params=pltpu.CompilerParams(
            collective_id=0, has_side_effects=True, vmem_limit_bytes=VMEM_LIMIT
        ),
        name="step",
    )(*operands)


def finish_kernel(*refs):
    sources, targets, sems = refs[:6], refs[6:12], refs[12]
    leave = [pltpu.make_async_copy(x, y, sems.at[i]) for i, (x, y) in enumerate(zip(sources, targets))]
    for copy in leave:
        copy.start()
    for copy in leave:
        copy.wait()


def finish(*results):
    inside = pl.BlockSpec(memory_space=pltpu.VMEM)
    outside = pl.BlockSpec(memory_space=pl.ANY)
    return pl.pallas_call(
        finish_kernel,
        out_shape=tuple(jax.ShapeDtypeStruct(r.shape, r.dtype) for r in results),
        in_specs=[inside] * 6,
        out_specs=(outside,) * 6,
        scratch_shapes=[pltpu.SemaphoreType.DMA((6,))],
        compiler_params=pltpu.CompilerParams(vmem_limit_bytes=4 * 1024 * 1024),
        name="finish",
    )(*results)


def local(
    video_tokens, audio_tokens, qkv_video, out_video, qkv_audio, out_audio, gain_video, gain_audio,
    time_from, time_to, time_steps, windows, intersection,
):
    d_video, d_audio, qv, qa, ov, oa = finish(*fused(
        time_steps, windows, intersection.swapaxes(1, 2), video_tokens[0], audio_tokens[0],
        gain_video.reshape(1, 2048), gain_audio.reshape(1, 2048), time_from, time_to,
        qkv_video.reshape(2048, 768), qkv_audio.reshape(2048, 768),
        out_video.reshape(256, 2048), out_audio.reshape(256, 2048),
    ))
    return d_video[None], d_audio[None], qv, ov.swapaxes(1, 2), qa, oa.swapaxes(1, 2)


def solution(mesh):
    return jax.shard_map(
        local,
        mesh=mesh,
        in_specs=(
            P("clip", "vid", None), P("clip", "vid", None), P(None, "aud", None), P("aud", None, None),
            P(None, "aud", None), P("aud", None, None), P(), P(), P(), P(),
            P("clip", None), P("clip", None), P("clip", None, None),
        ),
        out_specs=(
            P("clip", "vid", None), P("clip", "vid", None), P(("clip", "vid"), "aud", None),
            P("aud", None, ("clip", "vid")), P(("clip", "vid"), "aud", None), P("aud", None, ("clip", "vid")),
        ),
        check_vma=False,
    )
```

```python
import jax
import jax.numpy as jnp
from jax import lax
from jax.experimental import pallas as pl
from jax.experimental.pallas import tpu as pltpu
from jax.sharding import PartitionSpec as P

BLK = 32
TGRID = 64
STEPS = 2
EPSILON = 1e-06
MESH = pl.DeviceIdType.MESH
F32 = jnp.float32
BF16 = jnp.bfloat16
NT = (((1,), (1,)), ((), ()))
TN = (((0,), (0,)), ((), ()))
NN = (((1,), (0,)), ((), ()))
T1, ST, T2 = 0, 1, 2
GROUPS = 2
PIECE = 32 // GROUPS
VMEM_LIMIT = 42 * 1024 * 1024


def dot(a, b, dims):
    return lax.dot_general(a, b, dims, preferred_element_type=F32)


def kernel(
    steps, windows, ranges, xv, xa, gv, ga, tf, tt, wqv, wqa, wov, woa,
    dv_out, da_out, qv_out, qa_out, ov_out, oa_out,
    N0, NS, NG, NGT, OB, OG, GS, GG, DQ, DG, QR, KV, PS, PT, ACC,
    SB, R1, ZS, ZR, AG, DIFF, DO, DKV, DKS, DKR,
    WA, WR, WS, WF, WC, VR, VS, VF, MODS, BIAS,
    kv_s, kv_r, ar_s, ar_r, ng_s, ng_r, og_s, og_r, gg_s, gg_r,
    ed_s, ed_r, dg_s, dg_r, cl_s, cl_r, wf_r,
):
    v = lax.axis_index("vid")
    a = lax.axis_index("aud")
    c = lax.axis_index("clip")
    core = lax.rem(v, 2)
    yy = v // 2
    x = a // 2
    zh = lax.rem(a, 2)
    across = a + 1 - 2 * zh
    hops = (1, 3, 2)
    right = lax.rem(v + 1, 8)
    left = lax.rem(v + 7, 8)
    y_near = yy + 1 - 2 * lax.rem(yy, 2)
    y_far = 3 - yy
    y_one = (1 - core) * y_near + core * y_far
    y_two = core * y_near + (1 - core) * y_far
    y_last = 6 - yy - y_one - y_two
    mate = v + 1 - 2 * core

    def ahead(d):
        return lax.rem(x + d, 4)

    def piece(g, owner):
        return pl.ds(pl.multiple_of(PIECE * (4 * g + owner), PIECE), PIECE)

    chunks = [(g, m) for m in range(2) for g in range(GROUPS)]

    barrier = pltpu.get_barrier_semaphore()
    greet = [{"vid": lax.rem(v + d, 8)} for d in range(1, 8)]
    greet += [{"aud": peer} for peer in [2 * ahead(d) + zh for d in hops] + [across]]
    greet += [{"clip": c + 1 - 2 * lax.rem(c, 2)}]
    greet += [{"clip": lax.rem(c + 2, 4), "vid": 2 * yy + k} for k in range(2)]
    for peer in greet:
        pl.semaphore_signal(barrier, 1, device_id=peer, device_id_type=MESH)

    WQ = (wqv, wqa)
    WO = (wov, woa)
    pending = []

    def remote(src, dst, send, recv, device):
        return pltpu.make_async_remote_copy(
            src_ref=src, dst_ref=dst, send_sem=send, recv_sem=recv, device_id=device, device_id_type=MESH
        )

    def go(copy):
        copy.start()
        pending.append(copy)

    def wide(ref):
        return ref.astype(F32)

    now = steps[0, 0]
    stride = steps[0, 1]
    step = -stride.astype(F32) / TGRID
    conds = (
        tf[pl.ds(now, 1), :] + tt[pl.ds(now, 1), :],
        tf[pl.ds(now, 1), :] + tt[pl.ds(now - STEPS * stride, 1), :],
        tf[pl.ds(now - stride, 1), :] + tt[pl.ds(now - stride, 1), :],
    )
    gains = (gv, ga)
    for net in range(3):
        for m in range(2):
            MODS[2 * net + m : 2 * net + m + 1, :] = gains[m][...] * (1.0 + conds[net])

    xs = (xv, xa)

    def normed(net, m, r):
        part = pl.ds(pl.multiple_of(r * 32, 32), 32)
        cur = wide(xs[m][part, :])
        inv = lax.rsqrt(jnp.mean(cur * cur, -1, keepdims=True) + EPSILON)
        out = (cur * inv * MODS[2 * net + m : 2 * net + m + 1, :]).astype(BF16)
        N0[net, m, part, :] = out
        return part, out

    def make_qkv(net, rows, h, m):
        rounded = dot(rows, WQ[m][:, 384 * h : 384 * h + 384], NN).astype(BF16)
        QR[net, m, :, 128 * h : 128 * h + 128] = rounded[:, 0:128]
        KV[net, h, 1, m] = rounded[:, 128:384]

    def kv_copies(net, h, m):
        sent = KV.at[net, h, 1, m]
        return [
            remote(sent, KV.at[net, h, 2 * k, m], kv_s.at[net, h, m, k], kv_r.at[net, h, m, k], {"vid": device})
            for k, device in enumerate((right, left))
        ]

    def kv_start(net, h, m):
        for copy in kv_copies(net, h, m):
            go(copy)

    def kv_wait(net, h):
        for m in range(2):
            for copy in kv_copies(net, h, m):
                copy.wait_recv()

    for m in range(2):

        def norm_teacher(r, carry, m=m):
            normed(T1, m, r)
            return carry

        lax.fori_loop(0, 4, norm_teacher, 0)
    for m in range(2):
        make_qkv(T1, N0[T1, m], 0, m)
    pl.semaphore_wait(barrier, len(greet))
    for m in range(2):
        kv_start(T1, 0, m)
    for m in range(2):
        make_qkv(T1, N0[T1, m], 1, m)
        kv_start(T1, 1, m)

    for m in range(2):

        def norm_student(r, carry, m=m):
            part, student = normed(ST, m, r)
            for s in range(16):
                NS[m, s // 4, s % 4, part, :] = student[:, 128 * s : 128 * s + 128]
            return carry

        lax.fori_loop(0, 4, norm_student, 0)
    for h in range(2):
        for m in range(2):
            make_qkv(ST, N0[ST, m], h, m)
            kv_start(ST, h, m)

    qpos = lax.broadcasted_iota(jnp.int32, (128, 128), 0)
    kpos = lax.broadcasted_iota(jnp.int32, (128, 128), 1)
    qblk = lax.broadcasted_iota(jnp.int32, (128, 1), 0) // BLK
    kblk = lax.broadcasted_iota(jnp.int32, (1, 128), 1) // BLK

    def spans(which, first_block, block_of):
        out = jnp.zeros(block_of.shape, jnp.int32)
        for i in range(4):
            at = jnp.clip(first_block + i, 0, 31)
            out = jnp.where(block_of == i, ranges[0, which, at], out)
        return out

    low_q = spans(0, 4 * v, qblk)
    high_q = spans(1, 4 * v, qblk)
    for slot in range(3):
        shard = v + slot - 1
        at = kpos + 128 * shard
        inside = (at >= 0) & (at < 1024)
        apart = jnp.abs(qpos - (kpos + 128 * (slot - 1)))
        keys_at = kblk + 4 * shard
        low_k = spans(0, 4 * shard, kblk)
        high_k = spans(1, 4 * shard, kblk)
        query_at = qblk + 4 * v
        tests = (
            (apart < windows[0, 0], (keys_at >= low_q) & (keys_at < high_q)),
            ((query_at >= low_k) & (query_at < high_k), apart < windows[0, 1]),
        )
        for m in range(2):
            for k in range(2):
                cols = slice(256 * slot + 128 * k, 256 * slot + 128 * k + 128)
                BIAS[m, :, cols] = jnp.where(inside & tests[m][k], 0.0, -1e30)

    def spread(src, dst, send, recv, offsets):
        for d in offsets:
            peer = 2 * lax.rem(yy + d[0], 4) + lax.rem(core + d[1], 2)
            go(remote(src(lax.rem(peer, 2), peer // 2), dst.at[v], send.at[peer], recv.at[v], {"vid": peer}))

    def collect(dst, send, recv):
        for d in range(1, 8):
            peer = lax.rem(v + d, 8)
            remote(dst.at[peer], dst.at[peer], send.at[peer], recv.at[peer], {"vid": peer}).wait_recv()

    whole = [(0, 1), (1, 0), (3, 0), (1, 1), (3, 1), (2, 0), (2, 1)]

    factor = 128 ** (-0.5)

    def attention(net, m, h, save=False):
        queries = QR[net, m, :, 128 * h : 128 * h + 128]
        keys = KV[net, h, :, :, :, 0:128].reshape(768, 128)
        values = KV[net, h, :, :, :, 128:256].reshape(768, 128)
        scores = dot(queries, keys, NT) * factor + BIAS[m]
        shifted = jnp.exp(scores - jnp.max(scores, -1, keepdims=True))
        prob = shifted * (1.0 / jnp.sum(shifted, -1, keepdims=True))
        if save:
            PS[2 * m + h] = prob
        OB[net, m, :, 128 * h : 128 * h + 128] = dot(prob.astype(BF16), values, NN).astype(BF16)

    def project_out(net, m):
        return dot(OB[net, m], WO[m][...], NN)

    def over_x(i, g, m, d, src, dst, kind):
        return remote(src, dst, ar_s.at[i, g, m, kind + d], ar_r.at[i, g, m, kind + d], {"aud": 2 * ahead(d) + zh})

    def over_z(i, g, m):
        return remote(ZS.at[i, g, m], ZR.at[i, g, m], ar_s.at[i, g, m, 0], ar_r.at[i, g, m, 0], {"aud": across})

    def sum_start(i, m):
        for g in range(GROUPS):
            for d in hops:
                go(over_x(i, g, m, d, SB.at[i, m, piece(g, ahead(d))], R1.at[i, g, m, d - 1], 0))

    def sum_on(i):
        for g, m in chunks:
            total = wide(SB[i, m, piece(g, x), :])
            for d in hops:
                over_x(i, g, m, d, R1.at[i, g, m, d - 1], R1.at[i, g, m, d - 1], 0).wait_recv()
                total = total + wide(R1[i, g, m, d - 1])
            ZS[i, g, m] = total.astype(BF16)
            go(over_z(i, g, m))

    def summed(i, g, m):
        over_z(i, g, m).wait_recv()
        return wide(ZS[i, g, m]) + wide(ZR[i, g, m])

    def share(i, g, m, value):
        AG[i, m, piece(g, x), :] = value.astype(BF16)
        part = AG.at[i, m, piece(g, x)]
        for d in hops:
            go(over_x(i, g, m, d, part, part, 3))

    def share_end(i, m):
        for g in range(GROUPS):
            for d in hops:
                part = AG.at[i, m, piece(g, ahead(4 - d))]
                over_x(i, g, m, d, part, part, 3).wait_recv()

    kv_wait(T1, 0)
    for m in range(2):
        attention(T1, m, 0)
    kv_wait(T1, 1)
    for m in range(2):
        attention(T1, m, 1)
        field = project_out(T1, m)
        SB[0, m] = field.astype(BF16)
        sum_start(0, m)
        ACC[m] = -field
    for h in range(2):
        kv_wait(ST, h)
    NG[v] = NS[core, :, yy]
    spread(lambda k, y: NS.at[k, :, y], NG, ng_s, ng_r, whole)
    for m in range(2):
        for h in range(2):
            attention(ST, m, h, True)
    OG[v] = OB[ST, core]
    spread(lambda k, y: OB.at[ST, k], OG, og_s, og_r, whole)
    sum_on(0)
    for m in range(2):
        ACC[m] = ACC[m] + 2.0 * project_out(ST, m)
    for g, m in chunks:
        cur = wide(xs[m][piece(g, x), :]) + step * summed(0, g, m)
        inv = lax.rsqrt(jnp.mean(cur * cur, -1, keepdims=True) + EPSILON)
        share(0, g, m, cur * inv * MODS[4 + m : 5 + m, :])

    for m in range(2):
        share_end(0, m)
        for h in range(2):
            make_qkv(T2, AG[0, m], h, m)
            kv_start(T2, h, m)
    kv_wait(T2, 0)
    for m in range(2):
        attention(T2, m, 0)
    kv_wait(T2, 1)
    for m in range(2):
        attention(T2, m, 1)
        SB[1, m] = (ACC[m] - project_out(T2, m)).astype(BF16)
        sum_start(1, m)
    sum_on(1)
    for m in range(2):
        for h in range(2):
            PT[2 * m + h] = PS[2 * m + h].astype(BF16).T
    collect(NG, ng_s, ng_r)
    for s in range(4):
        NGT[128 * s : 128 * s + 128, :] = NG[:, s].reshape(1024, 128).T
    collect(OG, og_s, og_r)
    for g, m in chunks:
        diff = step * summed(1, g, m)
        DIFF[g, m] = diff
        share(1, g, m, 2.0 * step * diff)

    def backward(h, m):
        queries = QR[ST, m, :, 128 * h : 128 * h + 128]
        keys = KV[ST, h, :, :, :, 0:128].reshape(768, 128)
        values = KV[ST, h, :, :, :, 128:256].reshape(768, 128)
        grad_out = DO[m, :, 128 * h : 128 * h + 128]
        prob = PS[2 * m + h]
        grad_prob = dot(grad_out, values, NT)
        center = jnp.sum(prob * grad_prob, -1, keepdims=True)
        dscore = (prob * (grad_prob - center) * factor).astype(BF16)
        DQ[h, m, :, 0:128] = dot(dscore, keys, NN).astype(BF16)
        dkey = dot(dscore, queries, TN).reshape(3, 2, 128, 128)
        dvalue = dot(PT[2 * m + h], grad_out, NN).reshape(3, 2, 128, 128)
        if m == 0:
            DKV[h, :, :, :, 0:128] = dkey
            DKV[h, :, :, :, 128:256] = dvalue
        else:
            for slot in (0, 2):
                DKS[h, slot // 2, :, :, 0:128] = (DKV[h, slot, :, :, 0:128] + dkey[slot]).astype(BF16)
                DKS[h, slot // 2, :, :, 128:256] = (DKV[h, slot, :, :, 128:256] + dvalue[slot]).astype(BF16)
            DKV[h, 1, :, :, 0:128] = DKV[h, 1, :, :, 0:128] + dkey[1]
            DKV[h, 1, :, :, 128:256] = DKV[h, 1, :, :, 128:256] + dvalue[1]

    def edges(h):
        return [
            remote(DKS.at[h, k], DKR.at[h, k], ed_s.at[h, k], ed_r.at[h, k], {"vid": device})
            for k, device in enumerate((left, right))
        ]

    def finish_kv(h):
        for copy in edges(h):
            copy.wait_recv()
        for m in range(2):
            DQ[h, m, :, 128:384] = (DKV[h, 1, m] + wide(DKR[h, 0, m]) + wide(DKR[h, 1, m])).astype(BF16)

    def line(n, k, part, device):
        return remote(part, part, dg_s.at[n, k], dg_r.at[n, k], {"vid": device})

    def line_start(n):
        DG[n, yy, core] = DQ[n, core]
        go(remote(DQ.at[n, 1 - core], DG.at[n, yy, core], dg_s.at[n, 0], dg_r.at[n, 0], {"vid": mate}))

    def line_send(n):
        line(n, 0, DG.at[n, yy, 1 - core], mate).wait_recv()
        go(line(n, 1, DG.at[n, yy], 2 * y_one + core))
        go(line(n, 2, DG.at[n, yy], 2 * y_two + core))

    def line_on(n):
        line(n, 1, DG.at[n, y_one], 2 * y_one + core).wait_recv()
        go(line(n, 3, DG.at[n, y_one], 2 * y_two + core))

    def line_end(n):
        line(n, 2, DG.at[n, y_two], 2 * y_two + core).wait_recv()
        line(n, 3, DG.at[n, y_last], 2 * y_two + core).wait_recv()

    for m in range(2):
        share_end(1, m)
        DO[m] = dot(AG[1, m], WO[m][...], NT).astype(BF16)
        for h in range(2):
            backward(h, m)
            if m == 1:
                for copy in edges(h):
                    go(copy)
    finish_kv(0)
    line_start(0)
    for m in range(2):
        ACC[m] = dot(DQ[0, m], WQ[m][:, 0:384], NT)
    line_send(0)
    finish_kv(1)
    line_start(1)
    for m in range(2):
        SB[2, m] = (ACC[m] + dot(DQ[1, m], WQ[m][:, 384:768], NT)).astype(BF16)
        sum_start(2, m)
        if m == 0:
            line_send(1)
    line_on(0)

    c_one = c + 1 - 2 * lax.rem(c, 2)
    c_two = lax.rem(c + 2, 4)
    c_not = lax.rem(c_one + 2, 4)
    mine = pl.ds(pl.multiple_of(64 * core, 64), 64)
    theirs = pl.ds(pl.multiple_of(64 * (1 - core), 64), 64)

    parts = ((WA.at[0], WR.at[0], WS.at[0], WF.at[0]), (WA.at[1], WR.at[1], WS.at[1], WF.at[1]), (WC, VR, VS, VF))

    def clip_start(n):
        full, got, out, last = parts[n]
        for k, block in ((1, c_not), (0, c_one)):
            go(remote(full.at[block], got.at[k], cl_s.at[n, k], cl_r.at[n, k], {"clip": c_one}))

    def clip_on(n):
        full, got, out, last = parts[n]
        for k, block in ((1, c_two), (0, c)):
            part = got.at[k]
            remote(part, part, cl_s.at[n, k], cl_r.at[n, k], {"clip": c_one}).wait_recv()
            out[k] = (wide(full[block]) + wide(got[k])).astype(BF16)
            if k == 1:
                for j, half, device in ((2, mine, {"clip": c_two}), (3, theirs, {"clip": c_two, "vid": mate})):
                    go(remote(out.at[1, half], last.at[core, 1], cl_s.at[n, j], wf_r.at[n, core, 1], device))
            else:
                go(remote(out.at[0, theirs], last.at[core, 0], cl_s.at[n, 4], wf_r.at[n, core, 0], {"vid": mate}))
                last[core, 0] = out[0, mine, :]

    def clip_end(n):
        last = parts[n][3]
        for src, k, device in (
            (core, 1, {"clip": c_two}), (1 - core, 1, {"clip": c_two, "vid": mate}), (1 - core, 0, {"vid": mate})
        ):
            part = last.at[src, k]
            remote(part, part, cl_s.at[n, 2], wf_r.at[n, src, k], device).wait_recv()
        return [wide(last[m, 0]) + wide(last[m, 1]) for m in range(2)]

    def line_grad(n):
        line_end(n)
        WA[n] = dot(NGT[...], DG[n].reshape(1024, 384), NN).astype(BF16).reshape(4, 128, 384)
        clip_start(n)

    sum_on(2)
    line_on(1)
    for m in range(2):
        for s in range(16):
            GS[m, s // 4, s % 4] = AG[1, m, :, 128 * s : 128 * s + 128]
    GG[v] = GS[core, :, yy]
    spread(lambda k, y: GS.at[k, :, y], GG, gg_s, gg_r, whole)
    line_grad(0)
    def back_on(m):
        for g in range(GROUPS):
            cur = wide(xs[m][piece(g, x), :])
            inv = lax.rsqrt(jnp.mean(cur * cur, -1, keepdims=True) + EPSILON)
            scaled = summed(2, g, m) * MODS[2 + m : 3 + m, :]
            back = inv * scaled - cur * (inv * inv * inv) * jnp.mean(scaled * cur, -1, keepdims=True)
            share(2, g, m, DIFF[g, m] + back)

    back_on(0)
    line_grad(1)
    clip_on(0)
    back_on(1)
    collect(GG, gg_s, gg_r)
    o_all = OG[...].reshape(1024, 256)
    for s in range(4):
        WC[s] = dot(GG[:, s].reshape(1024, 128), o_all, TN).astype(BF16)
    clip_start(2)
    clip_on(1)
    clip_on(2)
    q_outs = (qv_out, qa_out)
    o_outs = (ov_out, oa_out)
    for h in range(2):
        for m, total in enumerate(clip_end(h)):
            q_outs[m][:, h, :] = total
    for m in range(2):
        share_end(2, m)
    dv_out[...] = AG[2, 0]
    da_out[...] = AG[2, 1]
    for m, total in enumerate(clip_end(2)):
        for h in range(2):
            o_outs[m][h] = total[:, 128 * h : 128 * h + 128]
    for copy in pending:
        copy.wait_send()


def vm(shape, kind=BF16):
    return pltpu.VMEM(shape, kind)


def fused(*operands):
    dma = pltpu.SemaphoreType.DMA
    inside = pl.BlockSpec(memory_space=pltpu.VMEM)
    scalar = pl.BlockSpec(memory_space=pltpu.SMEM)
    shape = jax.ShapeDtypeStruct
    return pl.pallas_call(
        kernel,
        out_shape=(
            shape((128, 2048), BF16), shape((128, 2048), BF16), shape((64, 2, 384), F32),
            shape((64, 2, 384), F32), shape((2, 64, 128), F32), shape((2, 64, 128), F32),
        ),
        in_specs=[scalar] * 3 + [inside] * 10,
        out_specs=(inside,) * 6,
        scratch_shapes=[
            vm((2, 2, 128, 2048)), vm((2, 4, 4, 128, 128)),
            vm((8, 4, 128, 128)), vm((512, 1024)), vm((3, 2, 128, 256)), vm((8, 128, 256)),
            vm((2, 4, 4, 128, 128)), vm((8, 4, 128, 128)), vm((2, 2, 128, 384)),
            vm((2, 4, 2, 128, 384)), vm((3, 2, 128, 256)),
            vm((3, 2, 3, 2, 128, 256)), vm((4, 128, 768), F32), vm((4, 768, 128)), vm((2, 128, 2048), F32),
            vm((3, 2, 128, 2048)), vm((3, GROUPS, 2, 3, PIECE, 2048)),
            vm((3, GROUPS, 2, PIECE, 2048)), vm((3, GROUPS, 2, PIECE, 2048)),
            vm((3, 2, 128, 2048)), vm((GROUPS, 2, PIECE, 2048), F32), vm((2, 128, 256)),
            vm((2, 3, 2, 128, 256), F32), vm((2, 2, 2, 128, 256)), vm((2, 2, 2, 128, 256)),
            vm((2, 4, 128, 384)), vm((2, 2, 128, 384)), vm((2, 2, 128, 384)), vm((2, 2, 2, 64, 384)),
            vm((4, 128, 256)), vm((2, 128, 256)), vm((2, 128, 256)), vm((2, 2, 64, 256)),
            vm((8, 2048), F32), vm((2, 128, 768), F32),
            dma((3, 2, 2, 2)), dma((3, 2, 2, 2)), dma((3, GROUPS, 2, 7)), dma((3, GROUPS, 2, 7)),
            dma((8,)), dma((8,)), dma((8,)), dma((8,)), dma((8,)), dma((8,)),
            dma((2, 2)), dma((2, 2)), dma((2, 4)), dma((2, 4)), dma((3, 5)), dma((3, 2)), dma((3, 2, 2)),
        ],
        compiler_params=pltpu.CompilerParams(
            collective_id=0, has_side_effects=True, vmem_limit_bytes=VMEM_LIMIT
        ),
        name="step",
    )(*operands)


def finish_kernel(*refs):
    sources, targets, sems = refs[:6], refs[6:12], refs[12]
    leave = [pltpu.make_async_copy(x, y, sems.at[i]) for i, (x, y) in enumerate(zip(sources, targets))]
    for copy in leave:
        copy.start()
    for copy in leave:
        copy.wait()


def finish(*results):
    inside = pl.BlockSpec(memory_space=pltpu.VMEM)
    outside = pl.BlockSpec(memory_space=pl.ANY)
    return pl.pallas_call(
        finish_kernel,
        out_shape=tuple(jax.ShapeDtypeStruct(r.shape, r.dtype) for r in results),
        in_specs=[inside] * 6,
        out_specs=(outside,) * 6,
        scratch_shapes=[pltpu.SemaphoreType.DMA((6,))],
        compiler_params=pltpu.CompilerParams(vmem_limit_bytes=4 * 1024 * 1024),
        name="finish",
    )(*results)


def local(
    video_tokens, audio_tokens, qkv_video, out_video, qkv_audio, out_audio, gain_video, gain_audio,
    time_from, time_to, time_steps, windows, intersection,
):
    d_video, d_audio, qv, qa, ov, oa = finish(*fused(
        time_steps, windows, intersection.swapaxes(1, 2), video_tokens[0], audio_tokens[0],
        gain_video.reshape(1, 2048), gain_audio.reshape(1, 2048), time_from, time_to,
        qkv_video.reshape(2048, 768), qkv_audio.reshape(2048, 768),
        out_video.reshape(256, 2048), out_audio.reshape(256, 2048),
    ))
    return d_video[None], d_audio[None], qv, ov.swapaxes(1, 2), qa, oa.swapaxes(1, 2)


def solution(mesh):
    return jax.shard_map(
        local,
        mesh=mesh,
        in_specs=(
            P("clip", "vid", None), P("clip", "vid", None), P(None, "aud", None), P("aud", None, None),
            P(None, "aud", None), P("aud", None, None), P(), P(), P(), P(),
            P("clip", None), P("clip", None), P("clip", None, None),
        ),
        out_specs=(
            P("clip", "vid", None), P("clip", "vid", None), P(("clip", "vid"), "aud", None),
            P("aud", None, ("clip", "vid")), P(("clip", "vid"), "aud", None), P("aud", None, ("clip", "vid")),
        ),
        check_vma=False,
    )
```
